32 devices in a mesh: batch: 2 (over x), time: 4 (over z), region: 4 (over y, core).
Axes of the slice: x: 2, y: 2, z: 4, core: 2. Of those that a mesh axis runs over, the one named last changes fastest.
Arguments:
- patches: bfloat16 [4096, 768], P(('batch', 'time', 'region')), parts along dimension 0
- enc_pos: bfloat16 [4096, 768], P(('batch', 'time', 'region')), parts along dimension 0
- vis_mask: int32 [4096], P(('batch', 'time', 'region')), parts along dimension 0
- dec_pos: bfloat16 [4096, 512], P(('batch', 'time', 'region')), parts along dimension 0
- w_embed: bfloat16 [768, 768], replicated
- b_embed: float32 [768], replicated
- enc_vec: float32 [2, 12, 768], replicated
- enc_wqkv: bfloat16 [2, 768, 3, 12, 64], replicated
- enc_wo: bfloat16 [2, 12, 64, 768], replicated
- enc_w1: bfloat16 [2, 768, 3072], replicated
- enc_w2: bfloat16 [2, 3072, 768], replicated
- enc_final: float32 [2, 768], replicated
- w_dec_in: bfloat16 [768, 512], replicated
- mask_token: bfloat16 [512], replicated
- dec_vec: float32 [2, 12, 512], replicated
- dec_wqkv: bfloat16 [2, 512, 3, 16, 32], replicated
- dec_wo: bfloat16 [2, 16, 32, 512], replicated
- dec_w1: bfloat16 [2, 512, 2048], replicated
- dec_w2: bfloat16 [2, 2048, 512], replicated
- dec_final: float32 [2, 512], replicated
- w_out: bfloat16 [512, 768], replicated
Outputs:
- output: float32 [4096, 768], P(('batch', 'time', 'region')), parts along dimension 0
There are 2 independent parts. The reference program is written for one: setup_inputs(seed, part) draws one part's arguments, and reference() takes and returns one part's arrays. A program takes and returns all parts, laid end to end along the dimension named above; an argument that names none is the same for every part.
All inputs are finite; a program needn't handle non-finite values.
Results may differ from the reference program's by a relative error of at most 0.0159007.
Values are sent between devices in bfloat16 or wider.
A program may use at most 1 GiB of HBM per device.

```python
import jax
import jax.numpy as jnp
from jax import lax

PATCH_DIM = 768
ENC_WIDTH = 768
ENC_HEADS = 12
DEC_WIDTH = 512
DEC_HEADS = 16
TOKENS_DEV = 128
TIME_BLOCKS = 4
REGIONS = 4
KEEP_DIV = 8
ENC_LAYERS = 2
DEC_LAYERS = 2

SHARDS = TIME_BLOCKS * REGIONS
TOKENS = TOKENS_DEV * SHARDS
VIS_DEV = TOKENS_DEV // KEEP_DIV
VISIBLE = VIS_DEV * SHARDS
SKEW = min(4, REGIONS)
ENC_HEAD = ENC_WIDTH // ENC_HEADS
DEC_HEAD = DEC_WIDTH // DEC_HEADS
LN_EPS = 1e-6


def draw_mask(mask_key):
    key_rank, key_shift, key_place = jax.random.split(mask_key, 3)
    pair_count = (REGIONS - SKEW) // 2
    shifts = jax.random.randint(key_shift, (TIME_BLOCKS, pair_count), 0, VIS_DEV + 1)
    paired = jnp.stack([VIS_DEV + shifts, VIS_DEV - shifts], axis=-1).reshape(TIME_BLOCKS, REGIONS - SKEW)
    profile = jnp.concatenate([jnp.full((TIME_BLOCKS, 1), SKEW * VIS_DEV, jnp.int32), jnp.zeros((TIME_BLOCKS, SKEW - 1), jnp.int32), paired.astype(jnp.int32)], axis=1)
    region_rank = jax.vmap(lambda one_key: jax.random.permutation(one_key, REGIONS))(jax.random.split(key_rank, TIME_BLOCKS))
    counts = jnp.take_along_axis(profile, region_rank, axis=1).reshape(SHARDS, 1)
    token_rank = jax.vmap(lambda one_key: jax.random.permutation(one_key, TOKENS_DEV))(jax.random.split(key_place, SHARDS))
    return (token_rank < counts).astype(jnp.int32).reshape(TOKENS)


def normal_draw(draw_key, out_shape, spread):
    return jax.random.normal(draw_key, out_shape, jnp.float32) * spread


def qkv_gain():
    return jnp.array([1.6, 1.6, 1.0], jnp.float32)[:, None, None]


def block_vectors(draw_key, layer_count, model_width):
    gain_rows = jnp.array([1.0, 0.0, 1.0, 0.0, 0.0, 0.0, 0.0, 0.0, 0.0, 0.0, 0.0, 0.0], jnp.float32)[:, None]
    return jax.random.normal(draw_key, (layer_count, 12, model_width), jnp.float32) * 0.2 + gain_rows


def final_vectors(draw_key, model_width):
    return jax.random.normal(draw_key, (2, model_width), jnp.float32) * 0.2 + jnp.array([1.0, 0.0], jnp.float32)[:, None]


def setup_inputs(seed: int = 0, part: int = 0) -> dict:
    part_key = jax.random.fold_in(jax.random.key(seed), part)
    key_patch, key_epos, key_mask, key_dpos = jax.random.split(part_key, 4)
    weight_keys = jax.random.split(jax.random.key(seed + 1), 17)
    return {
        "patches": normal_draw(key_patch, (TOKENS, PATCH_DIM), 1.0).astype(jnp.bfloat16),
        "enc_pos": normal_draw(key_epos, (TOKENS, ENC_WIDTH), 0.5).astype(jnp.bfloat16),
        "vis_mask": draw_mask(key_mask),
        "dec_pos": normal_draw(key_dpos, (TOKENS, DEC_WIDTH), 0.5).astype(jnp.bfloat16),
        "w_embed": normal_draw(weight_keys[0], (PATCH_DIM, ENC_WIDTH), PATCH_DIM ** -0.5).astype(jnp.bfloat16),
        "b_embed": normal_draw(weight_keys[1], (ENC_WIDTH,), 0.5),
        "enc_vec": block_vectors(weight_keys[2], ENC_LAYERS, ENC_WIDTH),
        "enc_wqkv": (normal_draw(weight_keys[3], (ENC_LAYERS, ENC_WIDTH, 3, ENC_HEADS, ENC_HEAD), ENC_WIDTH ** -0.5) * qkv_gain()).astype(jnp.bfloat16),
        "enc_wo": normal_draw(weight_keys[4], (ENC_LAYERS, ENC_HEADS, ENC_HEAD, ENC_WIDTH), 1.5 * ENC_WIDTH ** -0.5).astype(jnp.bfloat16),
        "enc_w1": normal_draw(weight_keys[5], (ENC_LAYERS, ENC_WIDTH, 4 * ENC_WIDTH), ENC_WIDTH ** -0.5).astype(jnp.bfloat16),
        "enc_w2": normal_draw(weight_keys[6], (ENC_LAYERS, 4 * ENC_WIDTH, ENC_WIDTH), (4 * ENC_WIDTH) ** -0.5).astype(jnp.bfloat16),
        "enc_final": final_vectors(weight_keys[7], ENC_WIDTH),
        "w_dec_in": normal_draw(weight_keys[8], (ENC_WIDTH, DEC_WIDTH), 1.5 * ENC_WIDTH ** -0.5).astype(jnp.bfloat16),
        "mask_token": normal_draw(weight_keys[9], (DEC_WIDTH,), 1.0).astype(jnp.bfloat16),
        "dec_vec": block_vectors(weight_keys[10], DEC_LAYERS, DEC_WIDTH),
        "dec_wqkv": (normal_draw(weight_keys[11], (DEC_LAYERS, DEC_WIDTH, 3, DEC_HEADS, DEC_HEAD), DEC_WIDTH ** -0.5) * qkv_gain()).astype(jnp.bfloat16),
        "dec_wo": normal_draw(weight_keys[12], (DEC_LAYERS, DEC_HEADS, DEC_HEAD, DEC_WIDTH), 1.5 * DEC_WIDTH ** -0.5).astype(jnp.bfloat16),
        "dec_w1": normal_draw(weight_keys[13], (DEC_LAYERS, DEC_WIDTH, 4 * DEC_WIDTH), DEC_WIDTH ** -0.5).astype(jnp.bfloat16),
        "dec_w2": normal_draw(weight_keys[14], (DEC_LAYERS, 4 * DEC_WIDTH, DEC_WIDTH), (4 * DEC_WIDTH) ** -0.5).astype(jnp.bfloat16),
        "dec_final": final_vectors(weight_keys[15], DEC_WIDTH),
        "w_out": normal_draw(weight_keys[16], (DEC_WIDTH, PATCH_DIM), DEC_WIDTH ** -0.5).astype(jnp.bfloat16),
    }


def layer_norm(hidden, ln_gain, ln_shift):
    hid_f32 = hidden.astype(jnp.float32)
    mean_val = jnp.mean(hid_f32, axis=-1, keepdims=True)
    centered = hid_f32 - mean_val
    variance = jnp.mean(centered * centered, axis=-1, keepdims=True)
    return centered * lax.rsqrt(variance + LN_EPS) * ln_gain + ln_shift


def attention(query_rows, key_rows, value_rows, blocks):
    query_count, head_count, head_dim = query_rows.shape
    q_blocks = query_rows.reshape(blocks, query_count // blocks, head_count, head_dim)
    key_f32 = key_rows.astype(jnp.float32)
    value_f32 = value_rows.astype(jnp.float32)

    def one_block(q_block):
        scores = jnp.einsum("qhd,khd->hqk", q_block.astype(jnp.float32), key_f32) * (head_dim ** -0.5)
        attn_probs = jax.nn.softmax(scores, axis=-1).astype(jnp.bfloat16)
        return jnp.einsum("hqk,khd->qhd", attn_probs.astype(jnp.float32), value_f32).astype(jnp.bfloat16)

    return lax.map(one_block, q_blocks).reshape(query_count, head_count, head_dim)


def transformer_block(hidden, vec_rows, w_qkv, w_o, w_one, w_two, blocks):
    head_count, head_dim = w_qkv.shape[2], w_qkv.shape[3]
    normed = layer_norm(hidden, vec_rows[0], vec_rows[1]).astype(jnp.bfloat16)
    qkv_bias = jnp.stack([vec_rows[4], jnp.zeros_like(vec_rows[4]), vec_rows[5]]).reshape(1, 3, head_count, head_dim)
    qkv_rows = (jnp.einsum("nd,dche->nche", normed.astype(jnp.float32), w_qkv.astype(jnp.float32)) + qkv_bias).astype(jnp.bfloat16)
    attended = attention(qkv_rows[:, 0], qkv_rows[:, 1], qkv_rows[:, 2], blocks)
    residual = (hidden.astype(jnp.float32) + jnp.einsum("nhe,hed->nd", attended.astype(jnp.float32), w_o.astype(jnp.float32)) + vec_rows[6]).astype(jnp.bfloat16)
    normed_mlp = layer_norm(residual, vec_rows[2], vec_rows[3]).astype(jnp.bfloat16)
    mlp_hidden = jax.nn.gelu(jnp.dot(normed_mlp, w_one, preferred_element_type=jnp.float32) + vec_rows[8:12].reshape(-1), approximate=False).astype(jnp.bfloat16)
    return (residual.astype(jnp.float32) + jnp.dot(mlp_hidden, w_two, preferred_element_type=jnp.float32) + vec_rows[7]).astype(jnp.bfloat16)


def run_stack(hidden, vec_stack, wqkv_stack, wo_stack, w1_stack, w2_stack, blocks):
    def layer_step(hidden_state, layer_params):
        vec_rows, w_qkv, w_o, w_one, w_two = layer_params
        return transformer_block(hidden_state, vec_rows, w_qkv, w_o, w_one, w_two, blocks), None

    final_state, _ = lax.scan(layer_step, hidden, (vec_stack, wqkv_stack, wo_stack, w1_stack, w2_stack))
    return final_state


def reference(patches, enc_pos, vis_mask, dec_pos, w_embed, b_embed, enc_vec, enc_wqkv, enc_wo, enc_w1, enc_w2, enc_final, w_dec_in, mask_token, dec_vec, dec_wqkv, dec_wo, dec_w1, dec_w2, dec_final, w_out):
    vis_idx = jnp.nonzero(vis_mask, size=VISIBLE)[0]
    embedded = (jnp.dot(patches[vis_idx], w_embed, preferred_element_type=jnp.float32) + b_embed + enc_pos[vis_idx].astype(jnp.float32)).astype(jnp.bfloat16)
    encoded = run_stack(embedded, enc_vec, enc_wqkv, enc_wo, enc_w1, enc_w2, SHARDS)
    latent = jnp.dot(layer_norm(encoded, enc_final[0], enc_final[1]).astype(jnp.bfloat16), w_dec_in, preferred_element_type=jnp.float32).astype(jnp.bfloat16)
    scattered = jnp.zeros((TOKENS, DEC_WIDTH), jnp.float32).at[vis_idx].set(latent.astype(jnp.float32))
    dec_in = (jnp.where(vis_mask[:, None] == 1, scattered, mask_token.astype(jnp.float32)) + dec_pos.astype(jnp.float32)).astype(jnp.bfloat16)
    decoded = run_stack(dec_in, dec_vec, dec_wqkv, dec_wo, dec_w1, dec_w2, SHARDS)
    return jnp.dot(layer_norm(decoded, dec_final[0], dec_final[1]).astype(jnp.bfloat16), w_out, preferred_element_type=jnp.float32)
```

```python
import functools
import jax
import jax.numpy as jnp
from jax import lax
from jax.experimental import pallas as pl
from jax.experimental.pallas import tpu as pltpu
from jax.sharding import PartitionSpec as P

LN_EPS = 1e-6
TOKEN_AXES = ("batch", "time", "region")
MESH = pl.DeviceIdType.MESH
F32 = jnp.float32
BF16 = jnp.bfloat16
LOG2E = 1.4426950408889634
BLK = 128
CODE = 144
SLOTS = 64
ZROWS = 128


def nn(a, b):
    return jnp.dot(a, b, preferred_element_type=F32)


def nt(a, b):
    return lax.dot_general(a, b, (((1,), (1,)), ((), ())), preferred_element_type=F32)


def tn(a, b):
    return lax.dot_general(a, b, (((0,), (0,)), ((), ())), preferred_element_type=F32)


def layer_norm(hidden, gain, shift):
    hid = hidden.astype(F32)
    mean = jnp.mean(hid, axis=-1, keepdims=True)
    centered = hid - mean
    var = jnp.mean(centered * centered, axis=-1, keepdims=True)
    return centered * lax.rsqrt(var + LN_EPS) * gain + shift


def gelu(x):
    return 0.5 * x * (1.0 + lax.erf(x * 0.7071067811865476))


class Peers:
    def __init__(self):
        self.z = lax.axis_index("time")
        self.r = lax.axis_index("region")
        self.core = lax.rem(self.r, 2)
        self.mate = self.r + 1 - 2 * self.core
        self.row = self.r // 2
        self.across = lax.rem(self.r + 2, 4)

    def zth(self, k):
        return lax.rem(self.z + k, 4)

    def ids(self):
        out = [{"time": self.z, "region": self.mate}, {"time": self.z, "region": self.across}]
        return out + [{"time": self.zth(k), "region": self.r} for k in (1, 2, 3)]

    def barrier(self):
        sem = pltpu.get_barrier_semaphore()
        for dev in self.ids():
            pl.semaphore_signal(sem, inc=1, device_id=dev, device_id_type=MESH)
        pl.semaphore_wait(sem, 5)


def remote(src, dst, sems, i, dev):
    return pltpu.make_async_remote_copy(
        src_ref=src, dst_ref=dst, send_sem=sems.at[0, i], recv_sem=sems.at[1, i],
        device_id=dev, device_id_type=MESH)


class Gather:
    COPIES = 15

    def __init__(self, peers, slots, sems):
        self.p, self.slots, self.sems = peers, slots, sems
        mate, across, *zs = peers.ids()
        self.mate, self.across, self.zs = mate, across, zs

    def copy(self, i, t, r, dev):
        block = self.slots.at[t, r]
        return remote(block, block, self.sems, i, dev)

    def start(self):
        p = self.p
        self.own = [self.copy(0, p.z, p.r, self.across)]
        self.own += [self.copy(k, p.z, p.r, self.zs[k - 1]) for k in (1, 2, 3)]
        self.own += [self.copy(4, p.z, p.r, self.mate)]
        for c in self.own:
            c.start()

    def forward_time(self):
        p = self.p
        self.fwd = []
        for k in (1, 3, 2):
            self.own[k].wait_recv()
            t = p.zth(4 - k)
            a = self.copy(4 + k, t, p.r, self.across)
            m = self.copy(7 + k, t, p.r, self.mate)
            a.start()
            m.start()
            self.fwd.append((k, a, m))

    def forward_across(self):
        p = self.p
        self.last = []
        self.own[0].wait_recv()
        c = self.copy(11, p.z, p.across, self.mate)
        c.start()
        self.last.append(c)
        for k, a, m in self.fwd:
            a.wait_recv()
            c = self.copy(11 + k, p.zth(4 - k), p.across, self.mate)
            c.start()
            self.last.append(c)

    def finish(self):
        self.own[4].wait_recv()
        for _, a, m in self.fwd:
            m.wait_recv()
        for c in self.last:
            c.wait_recv()
        for c in self.own:
            c.wait_send()
        for _, a, m in self.fwd:
            a.wait_send()
            m.wait_send()
        for c in self.last:
            c.wait_send()


def slot_codes(mask_row):
    n = mask_row.shape[1]
    upper = (lax.broadcasted_iota(jnp.int32, (n, n), 0) <= lax.broadcasted_iota(jnp.int32, (n, n), 1)).astype(F32)
    mask_f = jnp.broadcast_to(mask_row.astype(F32), (8, n))
    rank = nn(mask_f, upper)[0:1]
    return jnp.where(mask_row == 1, rank - 1.0, float(SLOTS))


def one_hot(code_row, rows):
    ids = lax.broadcasted_iota(jnp.int32, (rows, code_row.shape[1]), 0).astype(F32)
    return (ids == code_row).astype(BF16)


def enc_kernel(mask_ref, patches_ref, pos_ref, dpos_ref, b_embed_ref, vec_ref, fin_ref, w_embed_hbm, wqkv_hbm, wo_hbm, w1_hbm, w2_hbm, wdec_hbm,
               z_ref, dall_ref,
               w_embed, wqkv, wo, w1, w2, wdec, wsem,
               e_buf, p1_buf, e2_buf, p2_buf, f_all, att, xsem, gsem):
    p = Peers()
    loads = [pltpu.make_async_copy(w_embed_hbm, w_embed, wsem.at[0])]
    for l in range(2):
        for j, (src, dst) in enumerate(((wqkv_hbm, wqkv), (wo_hbm, wo), (w1_hbm, w1), (w2_hbm, w2))):
            loads.append(pltpu.make_async_copy(src.at[l], dst.at[l], wsem.at[1 + 4 * l + j]))
    loads.append(pltpu.make_async_copy(wdec_hbm, wdec, wsem.at[9]))
    for c in loads:
        c.start()
    p.barrier()

    code = slot_codes(mask_ref[...])
    sel = one_hot(code, SLOTS)
    picked = nn(sel, patches_ref[...]).astype(BF16)
    pos = nn(sel, pos_ref[...])
    have = jnp.sum(sel.astype(F32), axis=1, keepdims=True)
    loads[0].wait()
    emb = nn(picked, w_embed[...]) + b_embed_ref[...] + pos
    e_buf[...] = jnp.where(have > 0.5, emb, 0.0).astype(BF16)
    mate, across, *zs = p.ids()
    first = remote(e_buf, p1_buf, xsem, 0, mate)
    first.start()
    dall_ref[p.z, p.r, 0:BLK, :] = dpos_ref[...]
    dall_ref[p.z, p.r, BLK:CODE, :] = jnp.broadcast_to(jnp.concatenate([code, jnp.zeros((1, 384), F32)], axis=1), (CODE - BLK, 512)).astype(BF16)
    first.wait_recv()
    both = e_buf[...].astype(F32) + p1_buf[...].astype(F32)
    e2_buf[...] = both.astype(BF16).reshape(2, 32, 768)
    second = remote(e2_buf.at[p.core], p2_buf, xsem, 1, across)
    second.start()
    second.wait_recv()
    f_all[p.z, p.core] = (e2_buf[p.core].astype(F32) + p2_buf[...].astype(F32)).astype(BF16)
    own = f_all.at[p.z, p.core]
    thirds = [remote(own, own, xsem, 1 + k, zs[k - 1]) for k in (1, 2, 3)]
    for c in thirds:
        c.start()
    mates = [remote(own, own, xsem, 5, mate)]
    mates[0].start()
    gat = Gather(p, dall_ref, gsem)
    gat.start()
    for k in (1, 3, 2):
        thirds[k - 1].wait_recv()
        slot = f_all.at[p.zth(4 - k), p.core]
        c = remote(slot, slot, xsem, 5 + k, mate)
        c.start()
        mates.append(c)
    for c in mates:
        c.wait_recv()
    for c in [first, second] + thirds + mates:
        c.wait_send()

    h = f_all[...].reshape(256, 768)
    lane = lax.broadcasted_iota(jnp.int32, (256, 128), 1)
    for l in range(2):
        row = lambda i: vec_ref[i, l:l + 1, :]
        a = layer_norm(h, row(0), row(1)).astype(BF16)
        loads[1 + 4 * l].wait()
        q = nt(a, wqkv[l, 0:768]) + row(4)
        k = nt(a, wqkv[l, 768:1536]).astype(BF16)
        v = (nt(a, wqkv[l, 1536:2304]) + row(5)).astype(BF16)
        for g in range(6):
            cols = slice(128 * g, 128 * g + 128)
            outs = []
            for s in range(2):
                qm = jnp.where((lane // 64) == s, q[:, cols], 0.0).astype(BF16)
                sc = nt(qm, k[:, cols])
                top = jnp.max(sc, axis=-1, keepdims=True)
                pr = jnp.exp2((sc - top) * (0.125 * LOG2E))
                tot = jnp.sum(pr, axis=-1, keepdims=True)
                outs.append(nn(pr.astype(BF16), v[:, cols]) * (1.0 / tot))
            att[:, cols] = jnp.where(lane < 64, outs[0], outs[1]).astype(BF16)
        if l == 0:
            gat.forward_time()
        loads[2 + 4 * l].wait()
        res = (h.astype(F32) + nn(att[...], wo[l]) + row(6)).astype(BF16)
        b = layer_norm(res, row(2), row(3)).astype(BF16)
        acc = res.astype(F32) + row(7)
        loads[3 + 4 * l].wait()
        loads[4 + 4 * l].wait()
        for j in range(4):
            cols = slice(768 * j, 768 * j + 768)
            m = gelu(nn(b, w1[l, :, cols]) + row(8 + j)).astype(BF16)
            acc = acc + nn(m, w2[l, cols, :])
        h = acc.astype(BF16)
        if l == 0:
            gat.forward_across()
    loads[9].wait()
    zf = layer_norm(h, fin_ref[0:1, :], fin_ref[1:2, :]).astype(BF16)
    z_ref[...] = nn(zf, wdec[...]).astype(BF16).reshape(4, SLOTS, 512)
    gat.finish()


def dec_layer(l, h, kv_src, vec_ref, wqkv, wo, w1, w2, kt, vv, att, loads):
    row = lambda i: vec_ref[i, l:l + 1, :]
    q = nt(layer_norm(h, row(0), row(1)).astype(BF16), wqkv[l, 0:512]) + row(4)

    def project(j, carry):
        a = kv_src(j)
        kt[:, pl.ds(pl.multiple_of(j * 512, 512), 512)] = nt(wqkv[l, 512:1024], a).astype(BF16)
        vv[pl.ds(pl.multiple_of(j * 512, 512), 512), :] = (nt(a, wqkv[l, 1024:1536]) + row(5)).astype(BF16)
        return carry

    lax.fori_loop(0, 4, project, 0)
    lane = lax.broadcasted_iota(jnp.int32, (BLK, 128), 1)
    for g in range(4):
        cols = slice(128 * g, 128 * g + 128)
        acc = jnp.zeros((BLK, 128), F32)
        for s in range(4):
            qm = jnp.where((lane // 32) == s, q[:, cols], 0.0).astype(BF16)
            sc = nn(qm, kt[cols, :])
            top = jnp.max(sc, axis=-1, keepdims=True)
            pr = jnp.exp2((sc - top) * (32 ** -0.5 * LOG2E))
            tot = jnp.sum(pr, axis=-1, keepdims=True)
            o = nn(pr.astype(BF16), vv[:, cols]) * (1.0 / tot)
            acc = jnp.where((lane // 32) == s, o, acc)
        att[:, cols] = acc.astype(BF16)
    for c in loads:
        c.wait()
    res = (h.astype(F32) + nn(att[...], wo[l]) + row(6)).astype(BF16)
    b = layer_norm(res, row(2), row(3)).astype(BF16)
    acc = res.astype(F32) + row(7)
    for j in range(4):
        cols = slice(512 * j, 512 * j + 512)
        m = gelu(nn(b, w1[l, :, cols]) + row(8 + j)).astype(BF16)
        acc = acc + nn(m, w2[l, cols, :])
    return acc.astype(BF16)


def dec_kernel(mask_ref, dpos_ref, z_ref, dall_ref, mtok_ref, vec_ref, fin_ref, wqkv_hbm, wo_hbm, w1_hbm, w2_hbm,
               y_ref, wqkv, wo, w1, w2, wsem, table, a_all, kt, vv, att, gsem):
    p = Peers()
    loads = []
    for l in range(2):
        for j, (src, dst) in enumerate(((wqkv_hbm, wqkv), (wo_hbm, wo), (w1_hbm, w1), (w2_hbm, w2))):
            loads.append(pltpu.make_async_copy(src.at[l], dst.at[l], wsem.at[4 * l + j]))
    for c in loads:
        c.start()
    p.barrier()
    for t in range(4):
        table[t, 0:SLOTS, :] = z_ref[t]
        table[t, SLOTS:ZROWS, :] = jnp.broadcast_to(mtok_ref[...].astype(F32), (ZROWS - SLOTS, 512)).astype(BF16)

    def token_rows(code, t, dpos):
        return (tn(one_hot(code, ZROWS), table[t]) + dpos.astype(F32)).astype(BF16)

    h = token_rows(slot_codes(mask_ref[...]), p.z, dpos_ref[...])
    loads[0].wait()

    def first_src(j):
        rows = []
        for r in range(4):
            code = dall_ref[j, r, BLK:CODE, 0:BLK].astype(F32)[0:1]
            u = token_rows(code, j, dall_ref[j, r, 0:BLK, :])
            rows.append(layer_norm(u, vec_ref[0, 0:1, :], vec_ref[1, 0:1, :]).astype(BF16))
        return jnp.concatenate(rows, axis=0)

    h = dec_layer(0, h, first_src, vec_ref, wqkv, wo, w1, w2, kt, vv, att, loads[1:4])
    a_all[p.z, p.r] = layer_norm(h, vec_ref[0, 1:2, :], vec_ref[1, 1:2, :]).astype(BF16)
    gat = Gather(p, a_all, gsem)
    gat.start()
    loads[4].wait()
    gat.forward_time()
    gat.forward_across()
    gat.finish()
    h = dec_layer(1, h, lambda j: a_all[j].reshape(512, 512), vec_ref, wqkv, wo, w1, w2, kt, vv, att, loads[5:8])
    y_ref[...] = layer_norm(h, fin_ref[0:1, :], fin_ref[1:2, :]).astype(BF16)


VM = pl.BlockSpec(memory_space=pltpu.VMEM)
ANY = pl.BlockSpec(memory_space=pl.ANY)
DMA = pltpu.SemaphoreType.DMA


def solution(mesh):
    def local_step(patches, enc_pos, vis_mask, dec_pos, w_embed, b_embed, enc_vec, enc_wqkv, enc_wo, enc_w1, enc_w2, enc_final, w_dec_in, mask_token, dec_vec, dec_wqkv, dec_wo, dec_w1, dec_w2, dec_final, w_out):
        mask_row = vis_mask.reshape(1, BLK)
        wq_e = jnp.transpose(enc_wqkv, (0, 2, 3, 4, 1)).reshape(2, 2304, 768)
        wq_d = jnp.transpose(dec_wqkv, (0, 2, 3, 4, 1)).reshape(2, 1536, 512)
        wo_e = enc_wo.reshape(2, 768, 768)
        wo_d = dec_wo.reshape(2, 512, 512)
        z, dall = pl.pallas_call(
            enc_kernel,
            out_shape=(jax.ShapeDtypeStruct((4, SLOTS, 512), BF16), jax.ShapeDtypeStruct((4, 4, CODE, 512), BF16)),
            in_specs=[VM] * 7 + [ANY] * 6,
            out_specs=(VM, VM),
            scratch_shapes=[
                pltpu.VMEM((768, 768), BF16), pltpu.VMEM((2, 2304, 768), BF16), pltpu.VMEM((2, 768, 768), BF16),
                pltpu.VMEM((2, 768, 3072), BF16), pltpu.VMEM((2, 3072, 768), BF16), pltpu.VMEM((768, 512), BF16), DMA((10,)),
                pltpu.VMEM((64, 768), BF16), pltpu.VMEM((64, 768), BF16), pltpu.VMEM((2, 32, 768), BF16), pltpu.VMEM((32, 768), BF16),
                pltpu.VMEM((4, 2, 32, 768), BF16), pltpu.VMEM((256, 768), BF16), DMA((2, 9)), DMA((2, Gather.COPIES)),
            ],
            compiler_params=pltpu.CompilerParams(collective_id=0, has_side_effects=True, vmem_limit_bytes=60000 * 1024),
            name="encoder",
        )(mask_row, patches, enc_pos, dec_pos, b_embed.reshape(1, -1), jnp.transpose(enc_vec, (1, 0, 2)), enc_final, w_embed, wq_e, wo_e, enc_w1, enc_w2, w_dec_in)
        y = pl.pallas_call(
            dec_kernel,
            out_shape=jax.ShapeDtypeStruct((BLK, 512), BF16),
            in_specs=[VM] * 7 + [ANY] * 4,
            out_specs=VM,
            scratch_shapes=[
                pltpu.VMEM((2, 1536, 512), BF16), pltpu.VMEM((2, 512, 512), BF16),
                pltpu.VMEM((2, 512, 2048), BF16), pltpu.VMEM((2, 2048, 512), BF16), DMA((8,)),
                pltpu.VMEM((4, ZROWS, 512), BF16), pltpu.VMEM((4, 4, BLK, 512), BF16), pltpu.VMEM((512, 2048), BF16), pltpu.VMEM((2048, 512), BF16),
                pltpu.VMEM((BLK, 512), BF16), DMA((2, Gather.COPIES)),
            ],
            compiler_params=pltpu.CompilerParams(collective_id=1, has_side_effects=True, vmem_limit_bytes=60000 * 1024),
            name="decoder",
        )(mask_row, dec_pos, z, dall, mask_token.reshape(1, -1), jnp.transpose(dec_vec, (1, 0, 2)), dec_final, wq_d, wo_d, dec_w1, dec_w2)
        return jnp.dot(y, w_out, preferred_element_type=F32)

    token_rows = P(TOKEN_AXES, None)
    token_flags = P(TOKEN_AXES)
    replicated = P()
    in_specs = (token_rows, token_rows, token_flags, token_rows) + (replicated,) * 17
    return jax.shard_map(local_step, mesh=mesh, in_specs=in_specs, out_specs=token_rows, check_vma=False)
```

```python
import functools
import jax
import jax.numpy as jnp
from jax import lax
from jax.experimental import pallas as pl
from jax.experimental.pallas import tpu as pltpu
from jax.sharding import PartitionSpec as P

LN_EPS = 1e-6
TOKEN_AXES = ("batch", "time", "region")
MESH = pl.DeviceIdType.MESH
F32 = jnp.float32
BF16 = jnp.bfloat16
BLK = 128
CODE = 144
SLOTS = 64
ZROWS = 128


def nn(a, b):
    return jnp.dot(a, b, preferred_element_type=F32)


def nt(a, b):
    return lax.dot_general(a, b, (((1,), (1,)), ((), ())), preferred_element_type=F32)


def tn(a, b):
    return lax.dot_general(a, b, (((0,), (0,)), ((), ())), preferred_element_type=F32)


def layer_norm(hidden, gain, shift):
    hid = hidden.astype(F32)
    mean = jnp.mean(hid, axis=-1, keepdims=True)
    centered = hid - mean
    var = jnp.mean(centered * centered, axis=-1, keepdims=True)
    return centered * lax.rsqrt(var + LN_EPS) * gain + shift


def gelu(x):
    return 0.5 * x * (1.0 + lax.erf(x * 0.7071067811865476))


class Peers:
    def __init__(self):
        self.z = lax.axis_index("time")
        self.r = lax.axis_index("region")
        self.core = lax.rem(self.r, 2)
        self.mate = self.r + 1 - 2 * self.core
        self.row = self.r // 2
        self.across = lax.rem(self.r + 2, 4)
        self.inner = (self.z == 1) | (self.z == 2)
        self.mate_id = {"time": self.z, "region": self.mate}
        self.across_id = {"time": self.z, "region": self.across}
        self.near = {"time": self.z + 1 - 2 * lax.rem(self.z, 2), "region": self.r}
        self.far = {"time": 3 - self.z, "region": self.r}

    def zth(self, k):
        return lax.rem(self.z + k, 4)

    def ids(self):
        out = [{"time": self.z, "region": self.mate}, {"time": self.z, "region": self.across}]
        return out + [{"time": self.zth(k), "region": self.r} for k in (1, 2, 3)]

    def barrier(self):
        sem = pltpu.get_barrier_semaphore()
        for dev in self.ids():
            pl.semaphore_signal(sem, inc=1, device_id=dev, device_id_type=MESH)
        pl.semaphore_wait(sem, 5)


def remote(src, dst, sems, i, dev):
    return pltpu.make_async_remote_copy(
        src_ref=src, dst_ref=dst, send_sem=sems.at[0, i], recv_sem=sems.at[1, i],
        device_id=dev, device_id_type=MESH)


class Gather:
    def __init__(self, peers, slots, sends, recvs, rows, subs):
        self.p, self.slots, self.sends, self.recvs, self.rows, self.subs = peers, slots, sends, recvs, rows // subs, subs

    @staticmethod
    def sems(subs):
        return [DMA((5, 4, subs)), DMA((4, 4, subs))]

    def order(self, i):
        z = self.p.z
        hi = z // 2
        near = z + 1 - 2 * lax.rem(z, 2)
        if isinstance(i, int):
            return (z, near, 2 - hi, 3 - 3 * hi)[i]
        return jnp.where(i == 0, z, jnp.where(i == 1, near, jnp.where(i == 2, 2 - hi, 3 - 3 * hi)))

    def copy(self, send_kind, recv_kind, i, t, r, s, dev):
        block = self.slots.at[t, r, pl.ds(s * self.rows, self.rows)]
        return pltpu.make_async_remote_copy(
            src_ref=block, dst_ref=block, send_sem=self.sends.at[send_kind, i, s], recv_sem=self.recvs.at[recv_kind, t, s],
            device_id=dev, device_id_type=MESH)

    def near(self, i, t, s):
        return self.copy(0, 0, i, t, self.p.r, s, self.p.near)

    def far(self, i, t, s):
        return self.copy(1, 0, i, t, self.p.r, s, self.p.far)

    def cross(self, i, t, s):
        return self.copy(2, 1, i, t, self.p.r, s, self.p.across_id)

    def mate(self, i, t, s):
        return self.copy(3, 2, i, t, self.p.r, s, self.p.mate_id)

    def mate_across(self, i, t, s):
        return self.copy(4, 3, i, t, self.p.across, s, self.p.mate_id)

    def start(self):
        p = self.p
        for s in range(self.subs):
            self.near(0, p.z, s).start()

            @pl.when(p.inner)
            def _():
                self.far(0, p.z, s).start()

            self.cross(0, p.z, s).start()
            self.mate(0, p.z, s).start()

    def step(self, i):
        t = self.order(i)
        for s in range(self.subs):
            self.near(i, t, s).wait_recv()

            @pl.when(self.p.inner)
            def _():
                @pl.when(i == 1)
                def _():
                    self.far(i, t, s).start()

                @pl.when(i != 1)
                def _():
                    self.near(i, t, s).start()

            self.cross(i, t, s).start()
            self.mate(i, t, s).start()

    def pass_across(self, i):
        t = self.order(i)
        for s in range(self.subs):
            self.cross(i, t, s).wait_recv()
            self.mate_across(i, t, s).start()

    def wait_same(self, i):
        for s in range(self.subs):
            self.mate(i, self.order(i), s).wait_recv()

    def wait_across(self, i):
        for s in range(self.subs):
            self.mate_across(i, self.order(i), s).wait_recv()

    def finish(self):
        for i in range(4):
            t = self.order(i)
            for s in range(self.subs):
                if i == 0:
                    self.near(i, t, s).wait_send()

                @pl.when(self.p.inner)
                def _():
                    if i < 2:
                        self.far(i, t, s).wait_send()
                    else:
                        self.near(i, t, s).wait_send()

                self.cross(i, t, s).wait_send()
                self.mate(i, t, s).wait_send()
                self.mate_across(i, t, s).wait_send()


def slot_codes(mask_row):
    n = mask_row.shape[1]
    upper = (lax.broadcasted_iota(jnp.int32, (n, n), 0) <= lax.broadcasted_iota(jnp.int32, (n, n), 1)).astype(F32)
    mask_f = jnp.broadcast_to(mask_row.astype(F32), (8, n))
    rank = nn(mask_f, upper)[0:1]
    return jnp.where(mask_row == 1, rank - 1.0, float(SLOTS))


def one_hot(code_row, rows):
    ids = lax.broadcasted_iota(jnp.int32, (rows, code_row.shape[1]), 0).astype(F32)
    return (ids == code_row).astype(BF16)


def column(row):
    return jnp.transpose(jnp.broadcast_to(row, (128, row.shape[1])))


def attend(keys, vals, qtm, top_ref, tot_ref, acc_ref):
    n = keys.shape[0]
    ones = jnp.ones((16, n), BF16)
    scale = 32 ** -0.5

    def scores(pair):
        cols = slice(128 * (pair // 2), 128 * (pair // 2) + 128)
        return nn(keys[:, cols], qtm[pair])

    def update(pair, o, keep):
        tot_ref[pair:pair + 1, :] = tot_ref[pair:pair + 1, :] * keep + o[64:65]
        a, b = slice(64 * pair, 64 * pair + 32), slice(64 * pair + 32, 64 * pair + 64)
        acc_ref[a, :] = acc_ref[a, :] * keep[:, 0:128] + o[0:32, 0:128]
        acc_ref[b, :] = acc_ref[b, :] * keep[:, 128:256] + o[32:64, 128:256]

    sc = scores(0)
    late = None
    for pair in range(8):
        ahead = scores(pair + 1) if pair < 7 else None
        old = top_ref[pair:pair + 1, :]
        new = jnp.maximum(old, jnp.max(sc, axis=0, keepdims=True))
        pr = jnp.exp((sc - new) * scale).astype(BF16)
        keep = jnp.exp((old - new) * scale)
        top_ref[pair:pair + 1, :] = new
        o = nn(jnp.concatenate([vals[64 * pair:64 * pair + 64], ones], axis=0), pr)
        if late is not None:
            update(*late)
        late = (pair, o, keep)
        sc = ahead
    update(*late)


def dec_front(l, h, vec_ref, wqkv, qtm, vbias, top_ref, tot_ref, acc_ref):
    row = lambda i: vec_ref[i, l:l + 1, :]
    a = layer_norm(h, row(0), row(1)).astype(BF16)
    qt = (nt(wqkv[l, 0:512], a) + column(row(4))).astype(BF16)
    vbias[...] = column(row(5))
    qtm[...] = jnp.zeros((8, 128, 256), BF16)
    for head in range(16):
        base = 32 * (head % 4)
        qtm[head // 2, base:base + 32, 128 * (head % 2):128 * (head % 2) + 128] = qt[32 * head:32 * head + 32]
    top_ref[...] = jnp.full((8, 256), -jnp.inf, F32)
    tot_ref[...] = jnp.zeros((8, 256), F32)
    acc_ref[...] = jnp.zeros((512, 128), F32)
    return a


def dec_keys(l, a, wqkv, vbias):
    keys = nt(a, wqkv[l, 512:1024]).astype(BF16)
    vals = (nt(wqkv[l, 1024:1536], a) + jnp.concatenate([vbias[...]] * (a.shape[0] // 128), axis=1)).astype(BF16)
    return keys, vals


def dec_back(l, h, vec_ref, wo, w1, w2, tot_ref, acc_ref):
    row = lambda i: vec_ref[i, l:l + 1, :]
    parts = []
    for head in range(16):
        inv = 1.0 / tot_ref[head // 2:head // 2 + 1, 128 * (head % 2):128 * (head % 2) + 128]
        parts.append((acc_ref[32 * head:32 * head + 32, :] * inv).astype(BF16))
    att = jnp.concatenate(parts, axis=0)
    res = (h.astype(F32) + tn(att, wo[l]) + row(6)).astype(BF16)
    b = layer_norm(res, row(2), row(3)).astype(BF16)
    acc = res.astype(F32) + row(7)
    for j in range(4):
        cols = slice(512 * j, 512 * j + 512)
        m = gelu(nn(b, w1[l, :, cols]) + row(8 + j)).astype(BF16)
        acc = acc + nn(m, w2[l, cols, :])
    return acc.astype(BF16)


def kernel(mask_ref, patches_ref, pos_ref, dpos_ref, b_embed_ref, evec_ref, efin_ref, mtok_ref, dvec_ref, dfin_ref,
           w_embed_hbm, ewqkv_hbm, ewo_hbm, ew1_hbm, ew2_hbm, wdec_hbm, dwqkv_hbm, dwo_hbm, dw1_hbm, dw2_hbm,
           out_ref,
           w_embed, ewqkv, ewo, ew1, ew2, wdec, dwqkv, dwo, dw1, dw2, wsem,
           e_buf, p1_buf, e2_buf, p2_buf, f_all, att, xsem,
           dall, a_all, table, qtm, vbias, top_ref, tot_ref, acc_ref, s1, r1, s2, r2):
    p = Peers()
    loads = {}
    plan = [("embed", w_embed_hbm, w_embed)]
    for l in range(2):
        plan += [((n, l), src.at[l], dst.at[l]) for n, src, dst in (("eqkv", ewqkv_hbm, ewqkv), ("eo", ewo_hbm, ewo), ("e1", ew1_hbm, ew1), ("e2", ew2_hbm, ew2))]
    plan += [("dec", wdec_hbm, wdec)]
    for l in range(2):
        plan += [((n, l), src.at[l], dst.at[l]) for n, src, dst in (("dqkv", dwqkv_hbm, dwqkv), ("do", dwo_hbm, dwo), ("d1", dw1_hbm, dw1), ("d2", dw2_hbm, dw2))]
    for i, (name, src, dst) in enumerate(plan):
        loads[name] = pltpu.make_async_copy(src, dst, wsem.at[i])
        loads[name].start()
    code = slot_codes(mask_ref[...])
    sel = one_hot(code, SLOTS)
    picked = nn(sel, patches_ref[...]).astype(BF16)
    pos = nn(sel, pos_ref[...])
    have = jnp.sum(sel.astype(F32), axis=1, keepdims=True)
    loads["embed"].wait()
    emb = nn(picked, w_embed[...]) + b_embed_ref[...].reshape(1, 768) + pos
    e_buf[...] = jnp.where(have > 0.5, emb, 0.0).astype(BF16)
    dall[p.z, p.r, 0:BLK, :] = dpos_ref[...]
    dall[p.z, p.r, BLK:CODE, :] = jnp.broadcast_to(jnp.concatenate([code, jnp.zeros((1, 384), F32)], axis=1), (CODE - BLK, 512)).astype(BF16)
    p.barrier()
    mate, across, *zs = p.ids()
    first = remote(e_buf, p1_buf, xsem, 0, mate)
    first.start()
    first.wait_recv()
    both = e_buf[...].astype(F32) + p1_buf[...].astype(F32)
    e2_buf[...] = both.astype(BF16).reshape(2, 32, 768)
    second = remote(e2_buf.at[p.core], p2_buf, xsem, 1, across)
    second.start()
    second.wait_recv()
    f_all[p.z, p.core] = (e2_buf[p.core].astype(F32) + p2_buf[...].astype(F32)).astype(BF16)
    own = f_all.at[p.z, p.core]
    thirds = [remote(own, own, xsem, 1 + k, zs[k - 1]) for k in (1, 2, 3)]
    for c in thirds:
        c.start()
    mates = [remote(own, own, xsem, 5, mate)]
    mates[0].start()
    g1 = Gather(p, dall, s1, r1, CODE, 1)
    g1.start()
    for k in (1, 3, 2):
        thirds[k - 1].wait_recv()
        slot = f_all.at[p.zth(4 - k), p.core]
        c = remote(slot, slot, xsem, 5 + k, mate)
        c.start()
        mates.append(c)
    for c in mates:
        c.wait_recv()
    for c in [first, second] + thirds + mates:
        c.wait_send()
    h = f_all[...].reshape(256, 768)
    lane = lax.broadcasted_iota(jnp.int32, (256, 128), 1)
    for l in range(2):
        row = lambda i: evec_ref[i, l:l + 1, :]
        a = layer_norm(h, row(0), row(1)).astype(BF16)
        loads["eqkv", l].wait()
        q = nt(a, ewqkv[l, 0:768]) + row(4)
        k = nt(a, ewqkv[l, 768:1536]).astype(BF16)
        v = (nt(a, ewqkv[l, 1536:2304]) + row(5)).astype(BF16)
        for g in range(6):
            cols = slice(128 * g, 128 * g + 128)
            outs = []
            for s in range(2):
                qm = jnp.where((lane // 64) == s, q[:, cols], 0.0).astype(BF16)
                sc = nt(qm, k[:, cols])
                top = jnp.max(sc, axis=-1, keepdims=True)
                pr = jnp.exp((sc - top) * 0.125)
                tot = jnp.sum(pr, axis=-1, keepdims=True)
                outs.append(nn(pr.astype(BF16), v[:, cols]) * (1.0 / tot))
            att[:, cols] = jnp.where(lane < 64, outs[0], outs[1]).astype(BF16)
        if l == 0:
            g1.step(1)

            @pl.when(p.inner)
            def _():
                g1.step(2)

            g1.pass_across(0)
        else:
            @pl.when(p.inner)
            def _():
                g1.step(3)

            @pl.when(jnp.logical_not(p.inner))
            def _():
                g1.step(2)

            g1.pass_across(1)
        loads["eo", l].wait()
        res = (h.astype(F32) + nn(att[...], ewo[l]) + row(6)).astype(BF16)
        b = layer_norm(res, row(2), row(3)).astype(BF16)
        acc = res.astype(F32) + row(7)
        loads["e1", l].wait()
        loads["e2", l].wait()
        for j in range(4):
            cols = slice(768 * j, 768 * j + 768)
            m = gelu(nn(b, ew1[l, :, cols]) + row(8 + j)).astype(BF16)
            acc = acc + nn(m, ew2[l, cols, :])
        h = acc.astype(BF16)
        if l == 1:
            @pl.when(jnp.logical_not(p.inner))
            def _():
                g1.step(3)
    loads["dec"].wait()
    zf = layer_norm(h, efin_ref[0:1, :], efin_ref[1:2, :]).astype(BF16)
    table[:, 0:SLOTS, :] = nn(zf, wdec[...]).astype(BF16).reshape(4, SLOTS, 512)
    table[:, SLOTS:ZROWS, :] = jnp.broadcast_to(mtok_ref[...].astype(F32).reshape(1, 1, 512), (4, ZROWS - SLOTS, 512)).astype(BF16)
    def token_rows(code, t, dpos):
        return (tn(one_hot(code, ZROWS), table[t]) + dpos.astype(F32)).astype(BF16)

    h = token_rows(slot_codes(mask_ref[...]), p.z, dpos_ref[...])
    loads["dqkv", 0].wait()
    dec_front(0, h, dvec_ref, dwqkv, qtm, vbias, top_ref, tot_ref, acc_ref)
    def norm_rows(t, r):
        u = token_rows(dall[t, r, BLK:CODE, 0:BLK].astype(F32)[0:1], t, dall[t, r, 0:BLK, :])
        return layer_norm(u, dvec_ref[0, 0:1, :], dvec_ref[1, 0:1, :]).astype(BF16)

    def first_layer(i, carry):
        t = g1.order(i)

        @pl.when(i >= 2)
        def _():
            g1.pass_across(i)

        g1.wait_same(i)
        g1.wait_across(i)
        a = jnp.concatenate([norm_rows(t, r) for r in range(4)], axis=0)
        keys, vals = dec_keys(0, a, dwqkv, vbias)
        attend(keys, vals, qtm, top_ref, tot_ref, acc_ref)
        return carry
    lax.fori_loop(0, 4, first_layer, 0)
    for n in ("do", "d1", "d2"):
        loads[n, 0].wait()
    h = dec_back(0, h, dvec_ref, dwo, dw1, dw2, tot_ref, acc_ref)
    g1.finish()
    loads["dqkv", 1].wait()
    a_all[p.z, p.r] = dec_front(1, h, dvec_ref, dwqkv, qtm, vbias, top_ref, tot_ref, acc_ref)
    g2 = Gather(p, a_all, s2, r2, BLK, 2)
    g2.start()
    def second_layer(i, carry):
        t = g2.order(i)
        g2.wait_same(i)

        def chunk(half):
            ra = lax.rem(p.r + 2 * half, 4)
            rb = lax.rem(p.mate + 2 * half, 4)
            keys, vals = dec_keys(1, jnp.concatenate([a_all[t, ra], a_all[t, rb]], axis=0), dwqkv, vbias)
            attend(keys, vals, qtm, top_ref, tot_ref, acc_ref)

        chunk(0)

        @pl.when(i < 3)
        def _():
            g2.step(i + 1)

        g2.pass_across(i)
        g2.wait_across(i)
        chunk(1)
        return carry
    lax.fori_loop(0, 4, second_layer, 0)
    for n in ("do", "d1", "d2"):
        loads[n, 1].wait()
    h = dec_back(1, h, dvec_ref, dwo, dw1, dw2, tot_ref, acc_ref)
    out_ref[...] = layer_norm(h, dfin_ref[0:1, :], dfin_ref[1:2, :]).astype(BF16)
    g2.finish()


VM = pl.BlockSpec(memory_space=pltpu.VMEM)
ANY = pl.BlockSpec(memory_space=pl.ANY)
DMA = pltpu.SemaphoreType.DMA


def solution(mesh):
    def local_step(patches, enc_pos, vis_mask, dec_pos, w_embed, b_embed, enc_vec, enc_wqkv, enc_wo, enc_w1, enc_w2, enc_final, w_dec_in, mask_token, dec_vec, dec_wqkv, dec_wo, dec_w1, dec_w2, dec_final, w_out):
        mask_row = vis_mask.reshape(1, BLK)
        wq_e = jnp.transpose(enc_wqkv, (0, 2, 3, 4, 1)).reshape(2, 2304, 768)
        wq_d = jnp.transpose(dec_wqkv, (0, 2, 3, 4, 1)).reshape(2, 1536, 512)
        wo_e = enc_wo.reshape(2, 768, 768)
        wo_d = dec_wo.reshape(2, 512, 512)
        vm = lambda *shape: pltpu.VMEM(shape, BF16)
        vf = lambda *shape: pltpu.VMEM(shape, F32)
        y = pl.pallas_call(
            kernel,
            out_shape=jax.ShapeDtypeStruct((BLK, 512), BF16),
            in_specs=[VM] * 10 + [ANY] * 10,
            out_specs=VM,
            scratch_shapes=[
                vm(768, 768), vm(2, 2304, 768), vm(2, 768, 768), vm(2, 768, 3072), vm(2, 3072, 768), vm(768, 512),
                vm(2, 1536, 512), vm(2, 512, 512), vm(2, 512, 2048), vm(2, 2048, 512), DMA((18,)),
                vm(64, 768), vm(64, 768), vm(2, 32, 768), vm(32, 768), vm(4, 2, 32, 768), vm(256, 768), DMA((2, 9)),
                vm(4, 4, CODE, 512), vm(4, 4, BLK, 512), vm(4, ZROWS, 512), vm(8, 128, 256), vf(512, 128), vf(8, 256), vf(8, 256), vf(512, 128),
                *Gather.sems(1), *Gather.sems(2),
            ],
            compiler_params=pltpu.CompilerParams(collective_id=0, has_side_effects=True, vmem_limit_bytes=56 * 1024 * 1024),
            name="mae",
        )(mask_row, patches, enc_pos, dec_pos, b_embed, jnp.transpose(enc_vec, (1, 0, 2)), enc_final,
          mask_token, jnp.transpose(dec_vec, (1, 0, 2)), dec_final,
          w_embed, wq_e, wo_e, enc_w1, enc_w2, w_dec_in, wq_d, wo_d, dec_w1, dec_w2)
        return jnp.dot(y, w_out, preferred_element_type=F32)

    token_rows = P(TOKEN_AXES, None)
    token_flags = P(TOKEN_AXES)
    replicated = P()
    in_specs = (token_rows, token_rows, token_flags, token_rows) + (replicated,) * 17
    return jax.shard_map(local_step, mesh=mesh, in_specs=in_specs, out_specs=token_rows, check_vma=False)
```

```python
import functools
import jax
import jax.numpy as jnp
from jax import lax
from jax.experimental import pallas as pl
from jax.experimental.pallas import tpu as pltpu
from jax.sharding import PartitionSpec as P

LN_EPS = 1e-6
TOKEN_AXES = ("batch", "time", "region")
MESH = pl.DeviceIdType.MESH
F32 = jnp.float32
BF16 = jnp.bfloat16
BLK = 128
CODE = 144
SLOTS = 64
ZROWS = 128


def nn(a, b):
    return jnp.dot(a, b, preferred_element_type=F32)


def nt(a, b):
    return lax.dot_general(a, b, (((1,), (1,)), ((), ())), preferred_element_type=F32)


def tn(a, b):
    return lax.dot_general(a, b, (((0,), (0,)), ((), ())), preferred_element_type=F32)


def layer_norm(hidden, gain, shift):
    hid = hidden.astype(F32)
    mean = jnp.mean(hid, axis=-1, keepdims=True)
    centered = hid - mean
    var = jnp.mean(centered * centered, axis=-1, keepdims=True)
    return centered * lax.rsqrt(var + LN_EPS) * gain + shift


def gelu(x):
    return 0.5 * x * (1.0 + lax.erf(x * 0.7071067811865476))


class Peers:
    def __init__(self):
        self.z = lax.axis_index("time")
        self.r = lax.axis_index("region")
        self.core = lax.rem(self.r, 2)
        self.mate = self.r + 1 - 2 * self.core
        self.row = self.r // 2
        self.across = lax.rem(self.r + 2, 4)
        self.inner = (self.z == 1) | (self.z == 2)
        self.mate_id = {"time": self.z, "region": self.mate}
        self.across_id = {"time": self.z, "region": self.across}
        self.near = {"time": self.z + 1 - 2 * lax.rem(self.z, 2), "region": self.r}
        self.far = {"time": 3 - self.z, "region": self.r}

    def zth(self, k):
        return lax.rem(self.z + k, 4)

    def ids(self):
        out = [{"time": self.z, "region": self.mate}, {"time": self.z, "region": self.across}]
        return out + [{"time": self.zth(k), "region": self.r} for k in (1, 2, 3)]

    def greet(self):
        for dev in self.ids():
            pl.semaphore_signal(pltpu.get_barrier_semaphore(), inc=1, device_id=dev, device_id_type=MESH)

    def barrier(self):
        pl.semaphore_wait(pltpu.get_barrier_semaphore(), 5)


def remote(src, dst, sems, i, dev):
    return pltpu.make_async_remote_copy(
        src_ref=src, dst_ref=dst, send_sem=sems.at[0, i], recv_sem=sems.at[1, i],
        device_id=dev, device_id_type=MESH)


class Gather:
    def __init__(self, peers, slots, sends, recvs, rows, subs):
        self.p, self.slots, self.sends, self.recvs, self.rows, self.subs = peers, slots, sends, recvs, rows // subs, subs

    @staticmethod
    def sems(subs):
        return [DMA((5, 4, subs)), DMA((4, 4, subs))]

    def order(self, i):
        z = self.p.z
        hi = z // 2
        near = z + 1 - 2 * lax.rem(z, 2)
        if isinstance(i, int):
            return (z, near, 2 - hi, 3 - 3 * hi)[i]
        return jnp.where(i == 0, z, jnp.where(i == 1, near, jnp.where(i == 2, 2 - hi, 3 - 3 * hi)))

    def copy(self, send_kind, recv_kind, i, t, r, s, dev):
        block = self.slots.at[t, r, pl.ds(s * self.rows, self.rows)]
        return pltpu.make_async_remote_copy(
            src_ref=block, dst_ref=block, send_sem=self.sends.at[send_kind, i, s], recv_sem=self.recvs.at[recv_kind, t, s],
            device_id=dev, device_id_type=MESH)

    def near(self, i, t, s):
        return self.copy(0, 0, i, t, self.p.r, s, self.p.near)

    def far(self, i, t, s):
        return self.copy(1, 0, i, t, self.p.r, s, self.p.far)

    def cross(self, i, t, s):
        return self.copy(2, 1, i, t, self.p.r, s, self.p.across_id)

    def mate(self, i, t, s):
        return self.copy(3, 2, i, t, self.p.r, s, self.p.mate_id)

    def mate_across(self, i, t, s):
        return self.copy(4, 3, i, t, self.p.across, s, self.p.mate_id)

    def start(self):
        p = self.p
        for s in range(self.subs):
            self.near(0, p.z, s).start()

            @pl.when(p.inner)
            def _():
                self.far(0, p.z, s).start()

            self.cross(0, p.z, s).start()
            self.mate(0, p.z, s).start()

    def step(self, i):
        t = self.order(i)
        for s in range(self.subs):
            self.near(i, t, s).wait_recv()

            @pl.when(self.p.inner)
            def _():
                @pl.when(i == 1)
                def _():
                    self.far(i, t, s).start()

                @pl.when(i != 1)
                def _():
                    self.near(i, t, s).start()

            self.cross(i, t, s).start()
            self.mate(i, t, s).start()

    def pass_across(self, i):
        t = self.order(i)
        for s in range(self.subs):
            self.cross(i, t, s).wait_recv()
            self.mate_across(i, t, s).start()

    def wait_same(self, i):
        for s in range(self.subs):
            self.mate(i, self.order(i), s).wait_recv()

    def wait_across(self, i):
        for s in range(self.subs):
            self.mate_across(i, self.order(i), s).wait_recv()

    def finish(self):
        for i in range(4):
            t = self.order(i)
            for s in range(self.subs):
                if i == 0:
                    self.near(i, t, s).wait_send()

                @pl.when(self.p.inner)
                def _():
                    if i < 2:
                        self.far(i, t, s).wait_send()
                    else:
                        self.near(i, t, s).wait_send()

                self.cross(i, t, s).wait_send()
                self.mate(i, t, s).wait_send()
                self.mate_across(i, t, s).wait_send()


def slot_codes(mask_row):
    n = mask_row.shape[1]
    upper = (lax.broadcasted_iota(jnp.int32, (n, n), 0) <= lax.broadcasted_iota(jnp.int32, (n, n), 1)).astype(F32)
    mask_f = jnp.broadcast_to(mask_row.astype(F32), (8, n))
    rank = nn(mask_f, upper)[0:1]
    return jnp.where(mask_row == 1, rank - 1.0, float(SLOTS))


def one_hot(code_row, rows):
    ids = lax.broadcasted_iota(jnp.int32, (rows, code_row.shape[1]), 0).astype(F32)
    return (ids == code_row).astype(BF16)


def column(row):
    return jnp.transpose(jnp.broadcast_to(row, (128, row.shape[1])))


def attend(keys, vals, qtm, top_ref, tot_ref, acc_ref):
    n = keys.shape[0]
    ones = jnp.ones((16, n), BF16)
    scale = 32 ** -0.5

    def scores(pair):
        cols = slice(128 * (pair // 2), 128 * (pair // 2) + 128)
        return nn(keys[:, cols], qtm[pair])

    def update(pair, o, keep):
        tot_ref[pair:pair + 1, :] = tot_ref[pair:pair + 1, :] * keep + o[64:65]
        a, b = slice(64 * pair, 64 * pair + 32), slice(64 * pair + 32, 64 * pair + 64)
        acc_ref[a, :] = acc_ref[a, :] * keep[:, 0:128] + o[0:32, 0:128]
        acc_ref[b, :] = acc_ref[b, :] * keep[:, 128:256] + o[32:64, 128:256]

    sc = scores(0)
    late = None
    for pair in range(8):
        ahead = scores(pair + 1) if pair < 7 else None
        old = top_ref[pair:pair + 1, :]
        new = jnp.maximum(old, jnp.max(sc, axis=0, keepdims=True))
        pr = jnp.exp((sc - new) * scale).astype(BF16)
        keep = jnp.exp((old - new) * scale)
        top_ref[pair:pair + 1, :] = new
        o = nn(jnp.concatenate([vals[64 * pair:64 * pair + 64], ones], axis=0), pr)
        if late is not None:
            update(*late)
        late = (pair, o, keep)
        sc = ahead
    update(*late)


def dec_front(l, h, vec_ref, wqkv, qtm, vbias, top_ref, tot_ref, acc_ref):
    row = lambda i: vec_ref[i, l:l + 1, :]
    a = layer_norm(h, row(0), row(1)).astype(BF16)
    qt = (nt(wqkv[l, 0:512], a) + column(row(4))).astype(BF16)
    vbias[...] = column(row(5))
    qtm[...] = jnp.zeros((8, 128, 256), BF16)
    for head in range(16):
        base = 32 * (head % 4)
        qtm[head // 2, base:base + 32, 128 * (head % 2):128 * (head % 2) + 128] = qt[32 * head:32 * head + 32]
    top_ref[...] = jnp.full((8, 256), -jnp.inf, F32)
    tot_ref[...] = jnp.zeros((8, 256), F32)
    acc_ref[...] = jnp.zeros((512, 128), F32)
    return a


def dec_keys(l, a, wqkv, vbias):
    keys = nt(a, wqkv[l, 512:1024]).astype(BF16)
    vals = (nt(wqkv[l, 1024:1536], a) + jnp.concatenate([vbias[...]] * (a.shape[0] // 128), axis=1)).astype(BF16)
    return keys, vals


def dec_back(l, h, vec_ref, wo, w1, w2, tot_ref, acc_ref):
    row = lambda i: vec_ref[i, l:l + 1, :]
    parts = []
    for head in range(16):
        inv = 1.0 / tot_ref[head // 2:head // 2 + 1, 128 * (head % 2):128 * (head % 2) + 128]
        parts.append((acc_ref[32 * head:32 * head + 32, :] * inv).astype(BF16))
    att = jnp.concatenate(parts, axis=0)
    res = (h.astype(F32) + tn(att, wo[l]) + row(6)).astype(BF16)
    b = layer_norm(res, row(2), row(3)).astype(BF16)
    acc = res.astype(F32) + row(7)
    for j in range(4):
        cols = slice(512 * j, 512 * j + 512)
        m = gelu(nn(b, w1[l, :, cols]) + row(8 + j)).astype(BF16)
        acc = acc + nn(m, w2[l, cols, :])
    return acc.astype(BF16)


def kernel(mask_ref, patches_ref, pos_ref, dpos_ref, b_embed_ref, evec_ref, efin_ref, mtok_ref, dvec_ref, dfin_ref,
           w_embed_hbm, ewqkv_hbm, ewo_hbm, ew1_hbm, ew2_hbm, wdec_hbm, dwqkv_hbm, dwo_hbm, dw1_hbm, dw2_hbm,
           out_ref,
           w_embed, ewqkv, ewo, ew1, ew2, wdec, dwqkv, dwo, dw1, dw2, wsem,
           e_buf, p1_buf, e2_buf, p2_buf, f_all, att, xsem,
           dall, a_all, table, qtm, vbias, top_ref, tot_ref, acc_ref, s1, r1, s2, r2):
    p = Peers()
    p.greet()
    loads = {}
    plan = [("embed", w_embed_hbm, w_embed)]
    for l in range(2):
        plan += [((n, l), src.at[l], dst.at[l]) for n, src, dst in (("eqkv", ewqkv_hbm, ewqkv), ("eo", ewo_hbm, ewo), ("e1", ew1_hbm, ew1), ("e2", ew2_hbm, ew2))]
    plan += [("dec", wdec_hbm, wdec)]
    for l in range(2):
        plan += [((n, l), src.at[l], dst.at[l]) for n, src, dst in (("dqkv", dwqkv_hbm, dwqkv), ("do", dwo_hbm, dwo), ("d1", dw1_hbm, dw1), ("d2", dw2_hbm, dw2))]
    for i, (name, src, dst) in enumerate(plan):
        loads[name] = pltpu.make_async_copy(src, dst, wsem.at[i])
    loads["embed"].start()
    code = slot_codes(mask_ref[...])
    sel = one_hot(code, SLOTS)
    picked = nn(sel, patches_ref[...]).astype(BF16)
    pos = nn(sel, pos_ref[...])
    have = jnp.sum(sel.astype(F32), axis=1, keepdims=True)
    loads["embed"].wait()
    for name, *_ in plan[1:]:
        loads[name].start()
    emb = nn(picked, w_embed[...]) + b_embed_ref[...].reshape(1, 768) + pos
    e_buf[...] = jnp.where(have > 0.5, emb, 0.0).astype(BF16)
    dall[p.z, p.r, 0:BLK, :] = dpos_ref[...]
    dall[p.z, p.r, BLK:CODE, :] = jnp.broadcast_to(jnp.concatenate([code, jnp.zeros((1, 384), F32)], axis=1), (CODE - BLK, 512)).astype(BF16)
    p.barrier()
    mate, across, *zs = p.ids()
    first = remote(e_buf, p1_buf, xsem, 0, mate)
    first.start()
    first.wait_recv()
    both = e_buf[...].astype(F32) + p1_buf[...].astype(F32)
    e2_buf[...] = both.astype(BF16).reshape(2, 32, 768)
    second = remote(e2_buf.at[p.core], p2_buf, xsem, 1, across)
    second.start()
    second.wait_recv()
    f_all[p.z, p.core] = (e2_buf[p.core].astype(F32) + p2_buf[...].astype(F32)).astype(BF16)
    own = f_all.at[p.z, p.core]
    thirds = [remote(own, own, xsem, 1 + k, zs[k - 1]) for k in (1, 2, 3)]
    for c in thirds:
        c.start()
    mates = [remote(own, own, xsem, 5, mate)]
    mates[0].start()
    g1 = Gather(p, dall, s1, r1, CODE, 1)
    g1.start()
    for k in (1, 3, 2):
        thirds[k - 1].wait_recv()
        slot = f_all.at[p.zth(4 - k), p.core]
        c = remote(slot, slot, xsem, 5 + k, mate)
        c.start()
        mates.append(c)
    for c in mates:
        c.wait_recv()
    for c in [first, second] + thirds + mates:
        c.wait_send()
    h = f_all[...].reshape(256, 768)
    lane = lax.broadcasted_iota(jnp.int32, (256, 128), 1)
    for l in range(2):
        row = lambda i: evec_ref[i, l:l + 1, :]
        a = layer_norm(h, row(0), row(1)).astype(BF16)
        loads["eqkv", l].wait()
        q = nt(a, ewqkv[l, 0:768]) + row(4)
        k = nt(a, ewqkv[l, 768:1536]).astype(BF16)
        v = (nt(a, ewqkv[l, 1536:2304]) + row(5)).astype(BF16)
        for g in range(6):
            cols = slice(128 * g, 128 * g + 128)
            outs = []
            for s in range(2):
                qm = jnp.where((lane // 64) == s, q[:, cols], 0.0).astype(BF16)
                sc = nt(qm, k[:, cols])
                top = jnp.max(sc, axis=-1, keepdims=True)
                pr = jnp.exp((sc - top) * 0.125)
                tot = jnp.sum(pr, axis=-1, keepdims=True)
                outs.append(nn(pr.astype(BF16), v[:, cols]) * (1.0 / tot))
            att[:, cols] = jnp.where(lane < 64, outs[0], outs[1]).astype(BF16)
        if l == 0:
            g1.step(1)

            @pl.when(p.inner)
            def _():
                g1.step(2)

            g1.pass_across(0)
        else:
            @pl.when(p.inner)
            def _():
                g1.step(3)

            @pl.when(jnp.logical_not(p.inner))
            def _():
                g1.step(2)

            g1.pass_across(1)
        loads["eo", l].wait()
        res = (h.astype(F32) + nn(att[...], ewo[l]) + row(6)).astype(BF16)
        b = layer_norm(res, row(2), row(3)).astype(BF16)
        acc = res.astype(F32) + row(7)
        loads["e1", l].wait()
        loads["e2", l].wait()
        for j in range(4):
            cols = slice(768 * j, 768 * j + 768)
            m = gelu(nn(b, ew1[l, :, cols]) + row(8 + j)).astype(BF16)
            acc = acc + nn(m, ew2[l, cols, :])
        h = acc.astype(BF16)
    loads["dec"].wait()
    zf = layer_norm(h, efin_ref[0:1, :], efin_ref[1:2, :]).astype(BF16)
    table[:, 0:SLOTS, :] = nn(zf, wdec[...]).astype(BF16).reshape(4, SLOTS, 512)
    table[:, SLOTS:ZROWS, :] = jnp.broadcast_to(mtok_ref[...].astype(F32).reshape(1, 1, 512), (4, ZROWS - SLOTS, 512)).astype(BF16)
    def token_rows(code, t, dpos):
        return (tn(one_hot(code, ZROWS), table[t]) + dpos.astype(F32)).astype(BF16)

    h = token_rows(slot_codes(mask_ref[...]), p.z, dpos_ref[...])
    loads["dqkv", 0].wait()
    dec_front(0, h, dvec_ref, dwqkv, qtm, vbias, top_ref, tot_ref, acc_ref)

    @pl.when(jnp.logical_not(p.inner))
    def _():
        g1.step(3)
    def norm_rows(t, r):
        u = token_rows(dall[t, r, BLK:CODE, 0:BLK].astype(F32)[0:1], t, dall[t, r, 0:BLK, :])
        return layer_norm(u, dvec_ref[0, 0:1, :], dvec_ref[1, 0:1, :]).astype(BF16)

    def first_layer(i, carry):
        t = g1.order(i)

        @pl.when((i == 1) | (i == 2))
        def _():
            g1.pass_across(i + 1)

        g1.wait_same(i)
        g1.wait_across(i)
        a = jnp.concatenate([norm_rows(t, r) for r in range(4)], axis=0)
        keys, vals = dec_keys(0, a, dwqkv, vbias)
        attend(keys, vals, qtm, top_ref, tot_ref, acc_ref)
        return carry
    lax.fori_loop(0, 4, first_layer, 0)
    for n in ("do", "d1", "d2"):
        loads[n, 0].wait()
    h = dec_back(0, h, dvec_ref, dwo, dw1, dw2, tot_ref, acc_ref)
    g1.finish()
    loads["dqkv", 1].wait()
    a_all[p.z, p.r] = dec_front(1, h, dvec_ref, dwqkv, qtm, vbias, top_ref, tot_ref, acc_ref)
    g2 = Gather(p, a_all, s2, r2, BLK, 2)
    g2.start()
    def chunk(i, half):
        t = g2.order(i)
        ra = lax.rem(p.r + 2 * half, 4)
        rb = lax.rem(p.mate + 2 * half, 4)
        keys, vals = dec_keys(1, jnp.concatenate([a_all[t, ra], a_all[t, rb]], axis=0), dwqkv, vbias)
        attend(keys, vals, qtm, top_ref, tot_ref, acc_ref)

    def step_by_place(inner, outer):
        @pl.when(p.inner)
        def _():
            g2.step(inner)

        if outer:
            @pl.when(jnp.logical_not(p.inner))
            def _():
                g2.step(outer)
    g2.wait_same(0)
    chunk(0, 0)
    g2.step(1)
    g2.pass_across(0)
    step_by_place(2, 0)
    g2.wait_across(0)
    chunk(0, 1)
    step_by_place(3, 2)
    g2.wait_same(1)
    chunk(1, 0)
    g2.pass_across(1)
    g2.wait_same(2)
    chunk(2, 0)
    @pl.when(jnp.logical_not(p.inner))
    def _():
        g2.step(3)

    g2.wait_across(1)
    chunk(1, 1)
    g2.pass_across(2)
    g2.wait_same(3)
    chunk(3, 0)
    g2.wait_across(2)
    chunk(2, 1)
    g2.pass_across(3)
    g2.wait_across(3)
    chunk(3, 1)
    for n in ("do", "d1", "d2"):
        loads[n, 1].wait()
    h = dec_back(1, h, dvec_ref, dwo, dw1, dw2, tot_ref, acc_ref)
    out_ref[...] = layer_norm(h, dfin_ref[0:1, :], dfin_ref[1:2, :]).astype(BF16)
    g2.finish()


VM = pl.BlockSpec(memory_space=pltpu.VMEM)
ANY = pl.BlockSpec(memory_space=pl.ANY)
DMA = pltpu.SemaphoreType.DMA


def solution(mesh):
    def local_step(patches, enc_pos, vis_mask, dec_pos, w_embed, b_embed, enc_vec, enc_wqkv, enc_wo, enc_w1, enc_w2, enc_final, w_dec_in, mask_token, dec_vec, dec_wqkv, dec_wo, dec_w1, dec_w2, dec_final, w_out):
        mask_row = vis_mask.reshape(1, BLK)
        wq_e = jnp.transpose(enc_wqkv, (0, 2, 3, 4, 1)).reshape(2, 2304, 768)
        wq_d = jnp.transpose(dec_wqkv, (0, 2, 3, 4, 1)).reshape(2, 1536, 512)
        wo_e = enc_wo.reshape(2, 768, 768)
        wo_d = dec_wo.reshape(2, 512, 512)
        vm = lambda *shape: pltpu.VMEM(shape, BF16)
        vf = lambda *shape: pltpu.VMEM(shape, F32)
        y = pl.pallas_call(
            kernel,
            out_shape=jax.ShapeDtypeStruct((BLK, 512), BF16),
            in_specs=[VM] * 10 + [ANY] * 10,
            out_specs=VM,
            scratch_shapes=[
                vm(768, 768), vm(2, 2304, 768), vm(2, 768, 768), vm(2, 768, 3072), vm(2, 3072, 768), vm(768, 512),
                vm(2, 1536, 512), vm(2, 512, 512), vm(2, 512, 2048), vm(2, 2048, 512), DMA((18,)),
                vm(64, 768), vm(64, 768), vm(2, 32, 768), vm(32, 768), vm(4, 2, 32, 768), vm(256, 768), DMA((2, 9)),
                vm(4, 4, CODE, 512), vm(4, 4, BLK, 512), vm(4, ZROWS, 512), vm(8, 128, 256), vf(512, 128), vf(8, 256), vf(8, 256), vf(512, 128),
                *Gather.sems(1), *Gather.sems(2),
            ],
            compiler_params=pltpu.CompilerParams(collective_id=0, has_side_effects=True, vmem_limit_bytes=56 * 1024 * 1024),
            name="mae",
        )(mask_row, patches, enc_pos, dec_pos, b_embed, jnp.transpose(enc_vec, (1, 0, 2)), enc_final,
          mask_token, jnp.transpose(dec_vec, (1, 0, 2)), dec_final,
          w_embed, wq_e, wo_e, enc_w1, enc_w2, w_dec_in, wq_d, wo_d, dec_w1, dec_w2)
        return jnp.dot(y, w_out, preferred_element_type=F32)

    token_rows = P(TOKEN_AXES, None)
    token_flags = P(TOKEN_AXES)
    replicated = P()
    in_specs = (token_rows, token_rows, token_flags, token_rows) + (replicated,) * 17
    return jax.shard_map(local_step, mesh=mesh, in_specs=in_specs, out_specs=token_rows, check_vma=False)
```

```python
import functools
import jax
import jax.numpy as jnp
from jax import lax
from jax.experimental import pallas as pl
from jax.experimental.pallas import tpu as pltpu
from jax.sharding import PartitionSpec as P

LN_EPS = 1e-6
TOKEN_AXES = ("batch", "time", "region")
MESH = pl.DeviceIdType.MESH
F32 = jnp.float32
BF16 = jnp.bfloat16
BLK = 128
CODE = 144
SLOTS = 64
SUBS = 4
ZROWS = 128


def nn(a, b):
    return jnp.dot(a, b, preferred_element_type=F32)


def nt(a, b):
    return lax.dot_general(a, b, (((1,), (1,)), ((), ())), preferred_element_type=F32)


def tn(a, b):
    return lax.dot_general(a, b, (((0,), (0,)), ((), ())), preferred_element_type=F32)


def layer_norm(hidden, gain, shift):
    hid = hidden.astype(F32)
    mean = jnp.mean(hid, axis=-1, keepdims=True)
    centered = hid - mean
    var = jnp.mean(centered * centered, axis=-1, keepdims=True)
    return centered * lax.rsqrt(var + LN_EPS) * gain + shift


def gelu(x):
    return 0.5 * x * (1.0 + lax.erf(x * 0.7071067811865476))


class Peers:
    def __init__(self):
        self.z = lax.axis_index("time")
        self.r = lax.axis_index("region")
        self.core = lax.rem(self.r, 2)
        self.mate = self.r + 1 - 2 * self.core
        self.row = self.r // 2
        self.across = lax.rem(self.r + 2, 4)
        self.inner = (self.z == 1) | (self.z == 2)
        self.mate_id = {"time": self.z, "region": self.mate}
        self.across_id = {"time": self.z, "region": self.across}
        self.near = {"time": self.z + 1 - 2 * lax.rem(self.z, 2), "region": self.r}
        self.far = {"time": 3 - self.z, "region": self.r}

    def zth(self, k):
        return lax.rem(self.z + k, 4)

    def ids(self):
        out = [{"time": self.z, "region": self.mate}, {"time": self.z, "region": self.across}]
        return out + [{"time": self.zth(k), "region": self.r} for k in (1, 2, 3)]

    def greet(self):
        for dev in self.ids():
            pl.semaphore_signal(pltpu.get_barrier_semaphore(), inc=1, device_id=dev, device_id_type=MESH)

    def barrier(self):
        pl.semaphore_wait(pltpu.get_barrier_semaphore(), 5)


def remote(src, dst, sems, i, dev):
    return pltpu.make_async_remote_copy(
        src_ref=src, dst_ref=dst, send_sem=sems.at[0, i], recv_sem=sems.at[1, i],
        device_id=dev, device_id_type=MESH)


class Gather:
    def __init__(self, peers, slots, sends, recvs, mate_recvs, rows, subs):
        self.p, self.slots, self.sends, self.recvs, self.mate_recvs = peers, slots, sends, recvs, mate_recvs
        self.rows, self.subs = rows, subs

    @staticmethod
    def sems(subs, mates):
        return [DMA((5 if mates else 3, 4)), DMA((2, 4, subs)), DMA((2, 4))][:3 if mates else 2]

    def order(self, i):
        z = self.p.z
        hi = z // 2
        near = z + 1 - 2 * lax.rem(z, 2)
        if isinstance(i, int):
            return (z, near, 2 - hi, 3 - 3 * hi)[i]
        return jnp.where(i == 0, z, jnp.where(i == 1, near, jnp.where(i == 2, 2 - hi, 3 - 3 * hi)))

    def copy(self, send_kind, recv, i, t, r, s, dev):
        size = self.rows if s is None else self.rows // self.subs
        block = self.slots.at[t, r, pl.ds(0 if s is None else s * size, size)]
        return pltpu.make_async_remote_copy(
            src_ref=block, dst_ref=block, send_sem=self.sends.at[send_kind, i], recv_sem=recv, device_id=dev, device_id_type=MESH)

    def near(self, i, t, s=None):
        return self.copy(0, self.recvs.at[0, t, s or 0], i, t, self.p.r, s, self.p.near)

    def far(self, i, t, s=None):
        return self.copy(1, self.recvs.at[0, t, s or 0], i, t, self.p.r, s, self.p.far)

    def cross(self, i, t, s=None):
        return self.copy(2, self.recvs.at[1, t, s or 0], i, t, self.p.r, s, self.p.across_id)

    def mate(self, i, t, s=None):
        return self.copy(3, self.mate_recvs.at[0, t], i, t, self.p.r, s, self.p.mate_id)

    def mate_across(self, i, t, s=None):
        return self.copy(4, self.mate_recvs.at[1, t], i, t, self.p.across, s, self.p.mate_id)

    def start_line(self, s):
        self.near(0, self.p.z, s).start()

        @pl.when(self.p.inner)
        def _():
            self.far(0, self.p.z, s).start()

    def start_plane(self, s):
        self.cross(0, self.p.z, s).start()
        if self.mate_recvs is not None:
            self.mate(0, self.p.z, s).start()

    def step(self, i, s):
        t = self.order(i)
        self.near(i, t, s).wait_recv()

        @pl.when(self.p.inner)
        def _():
            @pl.when(i == 1)
            def _():
                self.far(i, t, s).start()

            @pl.when(i != 1)
            def _():
                self.near(i, t, s).start()

        self.cross(i, t, s).start()
        if self.mate_recvs is not None:
            self.mate(i, t, s).start()

    def pass_across(self, i, s):
        t = self.order(i)
        self.cross(i, t, s).wait_recv()
        if self.mate_recvs is not None:
            self.mate_across(i, t, s).start()

    def wait_same(self, i):
        self.mate(i, self.order(i)).wait_recv()

    def wait_across(self, i):
        self.mate_across(i, self.order(i)).wait_recv()

    def finish(self):
        self.near(0, self.p.z).wait_send()

        @pl.when(self.p.inner)
        def _():
            for i in range(4):
                (self.far if i < 2 else self.near)(i, self.order(i)).wait_send()

        for i in range(4):
            t = self.order(i)
            self.cross(i, t).wait_send()
            if self.mate_recvs is not None:
                self.mate(i, t).wait_send()
                self.mate_across(i, t).wait_send()


def slot_codes(mask_row):
    n = mask_row.shape[1]
    upper = (lax.broadcasted_iota(jnp.int32, (n, n), 0) <= lax.broadcasted_iota(jnp.int32, (n, n), 1)).astype(F32)
    mask_f = jnp.broadcast_to(mask_row.astype(F32), (8, n))
    rank = nn(mask_f, upper)[0:1]
    return jnp.where(mask_row == 1, rank - 1.0, float(SLOTS))


def one_hot(code_row, rows):
    ids = lax.broadcasted_iota(jnp.int32, (rows, code_row.shape[1]), 0).astype(F32)
    return (ids == code_row).astype(BF16)


def column(row):
    return jnp.transpose(jnp.broadcast_to(row, (128, row.shape[1])))


def attend(keys, vals, qtm, state):
    top_ref, tot_ref, acc_ref, sc_ref, pr_ref = state
    n = keys.shape[0]
    ones = jnp.ones((16, n), BF16)
    scale = 32 ** -0.5
    highs = []
    for pair in range(8):
        cols = slice(128 * (pair // 2), 128 * (pair // 2) + 128)
        sc = nn(keys[:, cols], qtm[pair])
        sc_ref[pair, 0:n] = sc
        highs.append(jnp.max(sc, axis=0, keepdims=True))
    keeps = []
    for pair in range(8):
        old = top_ref[pair:pair + 1, :]
        new = jnp.maximum(old, highs[pair])
        top_ref[pair:pair + 1, :] = new
        keeps.append(jnp.exp((old - new) * scale))
        pr_ref[pair, 0:n] = jnp.exp((sc_ref[pair, 0:n] - new) * scale).astype(BF16)
    for pair in range(8):
        o = nn(jnp.concatenate([vals[64 * pair:64 * pair + 64], ones], axis=0), pr_ref[pair, 0:n])
        keep = keeps[pair]
        tot_ref[pair:pair + 1, :] = tot_ref[pair:pair + 1, :] * keep + o[64:65]
        a, b = slice(64 * pair, 64 * pair + 32), slice(64 * pair + 32, 64 * pair + 64)
        acc_ref[a, :] = acc_ref[a, :] * keep[:, 0:128] + o[0:32, 0:128]
        acc_ref[b, :] = acc_ref[b, :] * keep[:, 128:256] + o[32:64, 128:256]


def dec_front(l, a, vec_ref, wqkv, qtm, vbias, top_ref, tot_ref, acc_ref):
    row = lambda i: vec_ref[i, l:l + 1, :]
    qt = (nt(wqkv[l, 0:512], a) + column(row(4))).astype(BF16)
    vbias[...] = column(row(5))
    qtm[...] = jnp.zeros((8, 128, 256), BF16)
    for head in range(16):
        base = 32 * (head % 4)
        qtm[head // 2, base:base + 32, 128 * (head % 2):128 * (head % 2) + 128] = qt[32 * head:32 * head + 32]
    top_ref[...] = jnp.full((8, 256), -jnp.inf, F32)
    tot_ref[...] = jnp.zeros((8, 256), F32)
    acc_ref[...] = jnp.zeros((512, 128), F32)


def dec_keys(l, a, wqkv, vbias):
    keys = nt(a, wqkv[l, 512:1024]).astype(BF16)
    vals = (nt(wqkv[l, 1024:1536], a) + jnp.concatenate([vbias[...]] * (a.shape[0] // 128), axis=1)).astype(BF16)
    return keys, vals


def dec_back(l, h, vec_ref, wo, w1, w2, tot_ref, acc_ref):
    row = lambda i: vec_ref[i, l:l + 1, :]
    parts = []
    for head in range(16):
        inv = 1.0 / tot_ref[head // 2:head // 2 + 1, 128 * (head % 2):128 * (head % 2) + 128]
        parts.append((acc_ref[32 * head:32 * head + 32, :] * inv).astype(BF16))
    att = jnp.concatenate(parts, axis=0)
    res = (h.astype(F32) + tn(att, wo[l]) + row(6)).astype(BF16)
    b = layer_norm(res, row(2), row(3)).astype(BF16)
    acc = res.astype(F32) + row(7)
    for j in range(4):
        cols = slice(512 * j, 512 * j + 512)
        m = gelu(nn(b, w1[l, :, cols]) + row(8 + j)).astype(BF16)
        acc = acc + nn(m, w2[l, cols, :])
    return acc.astype(BF16)


def kernel(mask_ref, patches_ref, pos_ref, dpos_ref, b_embed_ref, evec_ref, efin_ref, mtok_ref, dvec_ref, dfin_ref,
           w_embed_hbm, ewqkv_hbm, ewo_hbm, ew1_hbm, ew2_hbm, wdec_hbm, dwqkv_hbm, dwo_hbm, dw1_hbm, dw2_hbm,
           out_ref,
           w_embed, ewqkv, ewo, ew1, ew2, wdec, dwqkv, dwo, dw1, dw2, wsem,
           e_buf, p1_buf, e2_buf, p2_buf, f_all, att, xsem,
           dall, a_all, table, qtm, vbias, top_ref, tot_ref, acc_ref, sc_ref, pr_ref, s1, r1, m1, s2, r2, m2):
    p = Peers()
    p.greet()
    loads = {}
    state = (top_ref, tot_ref, acc_ref, sc_ref, pr_ref)
    plan = [("embed", w_embed_hbm, w_embed)]
    for l in range(2):
        plan += [((n, l), src.at[l], dst.at[l]) for n, src, dst in (("eqkv", ewqkv_hbm, ewqkv), ("eo", ewo_hbm, ewo), ("e1", ew1_hbm, ew1), ("e2", ew2_hbm, ew2))]
    plan += [("dec", wdec_hbm, wdec)]
    for l in range(2):
        plan += [((n, l), src.at[l], dst.at[l]) for n, src, dst in (("dqkv", dwqkv_hbm, dwqkv), ("do", dwo_hbm, dwo), ("d1", dw1_hbm, dw1), ("d2", dw2_hbm, dw2))]
    for i, (name, src, dst) in enumerate(plan):
        loads[name] = pltpu.make_async_copy(src, dst, wsem.at[i])
    loads["embed"].start()
    code = slot_codes(mask_ref[...])
    sel = one_hot(code, SLOTS)
    picked = nn(sel, patches_ref[...]).astype(BF16)
    pos = nn(sel, pos_ref[...])
    have = jnp.sum(sel.astype(F32), axis=1, keepdims=True)
    loads["embed"].wait()
    for name, *_ in plan[1:]:
        loads[name].start()
    emb = nn(picked, w_embed[...]) + b_embed_ref[...].reshape(1, 768) + pos
    e_buf[...] = jnp.where(have > 0.5, emb, 0.0).astype(BF16)
    dall[p.z, p.r, 0:BLK, :] = dpos_ref[...]
    dall[p.z, p.r, BLK:CODE, :] = jnp.broadcast_to(jnp.concatenate([code, jnp.zeros((1, 384), F32)], axis=1), (CODE - BLK, 512)).astype(BF16)
    p.barrier()
    mate, across, *zs = p.ids()
    first = remote(e_buf, p1_buf, xsem, 0, mate)
    first.start()
    first.wait_recv()
    both = e_buf[...].astype(F32) + p1_buf[...].astype(F32)
    e2_buf[...] = both.astype(BF16).reshape(2, 32, 768)
    second = remote(e2_buf.at[p.core], p2_buf, xsem, 1, across)
    second.start()
    second.wait_recv()
    f_all[p.z, p.core] = (e2_buf[p.core].astype(F32) + p2_buf[...].astype(F32)).astype(BF16)
    own = f_all.at[p.z, p.core]
    thirds = [remote(own, own, xsem, 1 + k, zs[k - 1]) for k in (1, 2, 3)]
    for c in thirds:
        c.start()
    mates = [remote(own, own, xsem, 5, mate)]
    mates[0].start()
    g1 = Gather(p, dall, s1, r1, m1, CODE, 1)
    g1.start_line(0)
    g1.start_plane(0)
    for k in (1, 3, 2):
        thirds[k - 1].wait_recv()
        slot = f_all.at[p.zth(4 - k), p.core]
        c = remote(slot, slot, xsem, 5 + k, mate)
        c.start()
        mates.append(c)
    for c in mates:
        c.wait_recv()
    for c in [first, second] + thirds + mates:
        c.wait_send()
    h = f_all[...].reshape(256, 768)
    lane = lax.broadcasted_iota(jnp.int32, (256, 128), 1)
    for l in range(2):
        row = lambda i: evec_ref[i, l:l + 1, :]
        a = layer_norm(h, row(0), row(1)).astype(BF16)
        loads["eqkv", l].wait()
        q = nt(a, ewqkv[l, 0:768]) + row(4)
        k = nt(a, ewqkv[l, 768:1536]).astype(BF16)
        v = (nt(a, ewqkv[l, 1536:2304]) + row(5)).astype(BF16)
        for g in range(6):
            cols = slice(128 * g, 128 * g + 128)
            outs = []
            for s in range(2):
                qm = jnp.where((lane // 64) == s, q[:, cols], 0.0).astype(BF16)
                sc = nt(qm, k[:, cols])
                top = jnp.max(sc, axis=-1, keepdims=True)
                pr = jnp.exp((sc - top) * 0.125)
                tot = jnp.sum(pr, axis=-1, keepdims=True)
                outs.append(nn(pr.astype(BF16), v[:, cols]) * (1.0 / tot))
            att[:, cols] = jnp.where(lane < 64, outs[0], outs[1]).astype(BF16)
        if l == 0:
            g1.step(1, 0)

            @pl.when(p.inner)
            def _():
                g1.step(2, 0)

            g1.pass_across(0, 0)
        else:
            @pl.when(p.inner)
            def _():
                g1.step(3, 0)

            @pl.when(jnp.logical_not(p.inner))
            def _():
                g1.step(2, 0)

            g1.pass_across(1, 0)
        loads["eo", l].wait()
        res = (h.astype(F32) + nn(att[...], ewo[l]) + row(6)).astype(BF16)
        b = layer_norm(res, row(2), row(3)).astype(BF16)
        acc = res.astype(F32) + row(7)
        loads["e1", l].wait()
        loads["e2", l].wait()
        for j in range(4):
            cols = slice(768 * j, 768 * j + 768)
            m = gelu(nn(b, ew1[l, :, cols]) + row(8 + j)).astype(BF16)
            acc = acc + nn(m, ew2[l, cols, :])
        h = acc.astype(BF16)
    loads["dec"].wait()
    zf = layer_norm(h, efin_ref[0:1, :], efin_ref[1:2, :]).astype(BF16)
    table[:, 0:SLOTS, :] = nn(zf, wdec[...]).astype(BF16).reshape(4, SLOTS, 512)
    table[:, SLOTS:ZROWS, :] = jnp.broadcast_to(mtok_ref[...].astype(F32).reshape(1, 1, 512), (4, ZROWS - SLOTS, 512)).astype(BF16)
    def token_rows(code, t, dpos):
        return (tn(one_hot(code, ZROWS), table[t]) + dpos.astype(F32)).astype(BF16)

    h = token_rows(slot_codes(mask_ref[...]), p.z, dpos_ref[...])
    loads["dqkv", 0].wait()
    dec_front(0, layer_norm(h, dvec_ref[0, 0:1, :], dvec_ref[1, 0:1, :]).astype(BF16), dvec_ref, dwqkv, qtm, vbias, top_ref, tot_ref, acc_ref)

    @pl.when(jnp.logical_not(p.inner))
    def _():
        g1.step(3, 0)
    def norm_rows(t, r):
        u = token_rows(dall[t, r, BLK:CODE, 0:BLK].astype(F32)[0:1], t, dall[t, r, 0:BLK, :])
        return layer_norm(u, dvec_ref[0, 0:1, :], dvec_ref[1, 0:1, :]).astype(BF16)

    def first_layer(i, carry):
        t = g1.order(i)

        @pl.when((i == 1) | (i == 2))
        def _():
            g1.pass_across(i + 1, 0)

        g1.wait_same(i)
        g1.wait_across(i)
        a = jnp.concatenate([norm_rows(t, r) for r in range(4)], axis=0)
        keys, vals = dec_keys(0, a, dwqkv, vbias)
        attend(keys, vals, qtm, state)
        return carry
    lax.fori_loop(0, 4, first_layer, 0)
    for n in ("do", "d1", "d2"):
        loads[n, 0].wait()
    h = dec_back(0, h, dvec_ref, dwo, dw1, dw2, tot_ref, acc_ref)
    g1.finish()
    a_all[p.z, p.r] = layer_norm(h, dvec_ref[0, 1:2, :], dvec_ref[1, 1:2, :]).astype(BF16)
    g2 = Gather(p, a_all, s2, r2, m2, BLK, SUBS)
    for s in range(SUBS):
        g2.start_line(s)
        g2.start_plane(s)
    loads["dqkv", 1].wait()
    dec_front(1, a_all[p.z, p.r], dvec_ref, dwqkv, qtm, vbias, top_ref, tot_ref, acc_ref)
    def chunk(i, half):
        t = g2.order(i)
        ra = lax.rem(p.r + 2 * half, 4)
        rb = lax.rem(p.mate + 2 * half, 4)
        keys, vals = dec_keys(1, jnp.concatenate([a_all[t, ra], a_all[t, rb]], axis=0), dwqkv, vbias)
        attend(keys, vals, qtm, state)

    def outer_step(i, s):
        @pl.when(jnp.logical_not(p.inner))
        def _():
            g2.step(i, s)

    def inner_step(i, s):
        @pl.when(p.inner)
        def _():
            g2.step(i, s)
    g2.wait_same(0)
    chunk(0, 0)
    for s in range(SUBS):
        g2.step(1, s)
        inner_step(2, s)
        g2.pass_across(0, s)
    for s in range(SUBS):
        inner_step(3, s)
    g2.wait_across(0)
    chunk(0, 1)
    for s in range(SUBS):
        outer_step(2, s)
    g2.wait_same(1)
    chunk(1, 0)
    for s in range(SUBS):
        g2.pass_across(1, s)
    g2.wait_same(2)
    chunk(2, 0)
    for s in range(SUBS):
        outer_step(3, s)
    g2.wait_across(1)
    chunk(1, 1)
    for s in range(SUBS):
        g2.pass_across(2, s)
    g2.wait_same(3)
    chunk(3, 0)
    g2.wait_across(2)
    chunk(2, 1)
    for s in range(SUBS):
        g2.pass_across(3, s)
    g2.wait_across(3)
    chunk(3, 1)
    for n in ("do", "d1", "d2"):
        loads[n, 1].wait()
    h = dec_back(1, h, dvec_ref, dwo, dw1, dw2, tot_ref, acc_ref)
    out_ref[...] = layer_norm(h, dfin_ref[0:1, :], dfin_ref[1:2, :]).astype(BF16)
    g2.finish()


VM = pl.BlockSpec(memory_space=pltpu.VMEM)
ANY = pl.BlockSpec(memory_space=pl.ANY)
DMA = pltpu.SemaphoreType.DMA


def solution(mesh):
    def local_step(patches, enc_pos, vis_mask, dec_pos, w_embed, b_embed, enc_vec, enc_wqkv, enc_wo, enc_w1, enc_w2, enc_final, w_dec_in, mask_token, dec_vec, dec_wqkv, dec_wo, dec_w1, dec_w2, dec_final, w_out):
        mask_row = vis_mask.reshape(1, BLK)
        wq_e = jnp.transpose(enc_wqkv, (0, 2, 3, 4, 1)).reshape(2, 2304, 768)
        wq_d = jnp.transpose(dec_wqkv, (0, 2, 3, 4, 1)).reshape(2, 1536, 512)
        wo_e = enc_wo.reshape(2, 768, 768)
        wo_d = dec_wo.reshape(2, 512, 512)
        vm = lambda *shape: pltpu.VMEM(shape, BF16)
        vf = lambda *shape: pltpu.VMEM(shape, F32)
        y = pl.pallas_call(
            kernel,
            out_shape=pltpu.VMEM((BLK, 512), BF16),
            in_specs=[VM] * 10 + [ANY] * 10,
            out_specs=VM,
            scratch_shapes=[
                vm(768, 768), vm(2, 2304, 768), vm(2, 768, 768), vm(2, 768, 3072), vm(2, 3072, 768), vm(768, 512),
                vm(2, 1536, 512), vm(2, 512, 512), vm(2, 512, 2048), vm(2, 2048, 512), DMA((18,)),
                vm(64, 768), vm(64, 768), vm(2, 32, 768), vm(32, 768), vm(4, 2, 32, 768), vm(256, 768), DMA((2, 9)),
                vm(4, 4, CODE, 512), vm(4, 4, BLK, 512), vm(4, ZROWS, 512), vm(8, 128, 256), vf(512, 128), vf(8, 256), vf(8, 256), vf(512, 128), vf(8, 512, 256), vm(8, 512, 256),
                *Gather.sems(1, True), *Gather.sems(SUBS, True),
            ],
            compiler_params=pltpu.CompilerParams(collective_id=0, has_side_effects=True, vmem_limit_bytes=60 * 1024 * 1024),
            name="mae",
        )(mask_row, patches, enc_pos, dec_pos, b_embed, jnp.transpose(enc_vec, (1, 0, 2)), enc_final,
          mask_token, jnp.transpose(dec_vec, (1, 0, 2)), dec_final,
          w_embed, wq_e, wo_e, enc_w1, enc_w2, w_dec_in, wq_d, wo_d, dec_w1, dec_w2)
        return jnp.dot(y, w_out, preferred_element_type=F32)

    token_rows = P(TOKEN_AXES, None)
    token_flags = P(TOKEN_AXES)
    replicated = P()
    in_specs = (token_rows, token_rows, token_flags, token_rows) + (replicated,) * 17
    return jax.shard_map(local_step, mesh=mesh, in_specs=in_specs, out_specs=token_rows, check_vma=False)
```

```python
import functools
import jax
import jax.numpy as jnp
from jax import lax
from jax.experimental import pallas as pl
from jax.experimental.pallas import tpu as pltpu
from jax.sharding import PartitionSpec as P

LN_EPS = 1e-6
TOKEN_AXES = ("batch", "time", "region")
MESH = pl.DeviceIdType.MESH
F32 = jnp.float32
BF16 = jnp.bfloat16
BLK = 128
CODE = 144
E = 768
D = 512
SLOTS = 64
SUBS = 4
ZROWS = 128


def nn(a, b):
    return jnp.dot(a, b, preferred_element_type=F32)


def nt(a, b):
    return lax.dot_general(a, b, (((1,), (1,)), ((), ())), preferred_element_type=F32)


def tn(a, b):
    return lax.dot_general(a, b, (((0,), (0,)), ((), ())), preferred_element_type=F32)


def layer_norm(hidden, gain, shift):
    hid = hidden.astype(F32)
    mean = jnp.mean(hid, axis=-1, keepdims=True)
    centered = hid - mean
    var = jnp.mean(centered * centered, axis=-1, keepdims=True)
    return centered * lax.rsqrt(var + LN_EPS) * gain + shift


def gelu(x):
    return 0.5 * x * (1.0 + lax.erf(x * 0.7071067811865476))


class Peers:
    def __init__(self):
        self.z = lax.axis_index("time")
        self.r = lax.axis_index("region")
        self.core = lax.rem(self.r, 2)
        self.mate = self.r + 1 - 2 * self.core
        self.row = self.r // 2
        self.across = lax.rem(self.r + 2, 4)
        self.inner = (self.z == 1) | (self.z == 2)
        self.mate_id = {"time": self.z, "region": self.mate}
        self.across_id = {"time": self.z, "region": self.across}
        self.near = {"time": self.z + 1 - 2 * lax.rem(self.z, 2), "region": self.r}
        self.far = {"time": 3 - self.z, "region": self.r}

    def zth(self, k):
        return lax.rem(self.z + k, 4)

    def ids(self):
        out = [{"time": self.z, "region": self.mate}, {"time": self.z, "region": self.across}]
        return out + [{"time": self.zth(k), "region": self.r} for k in (1, 2, 3)]

    def greet(self):
        for dev in self.ids():
            pl.semaphore_signal(pltpu.get_barrier_semaphore(), inc=1, device_id=dev, device_id_type=MESH)

    def barrier(self):
        pl.semaphore_wait(pltpu.get_barrier_semaphore(), 5)


def remote(src, dst, sems, i, dev):
    return pltpu.make_async_remote_copy(
        src_ref=src, dst_ref=dst, send_sem=sems.at[0, i], recv_sem=sems.at[1, i],
        device_id=dev, device_id_type=MESH)


class Gather:
    def __init__(self, peers, slots, sends, recvs, mate_recvs, rows, subs):
        self.p, self.slots, self.sends, self.recvs, self.mate_recvs = peers, slots, sends, recvs, mate_recvs
        self.rows, self.subs = rows, subs

    @staticmethod
    def sems(subs, mates):
        return [DMA((5 if mates else 3, 4)), DMA((2, 4, subs)), DMA((2, 4))][:3 if mates else 2]

    def order(self, i):
        z = self.p.z
        hi = z // 2
        near = z + 1 - 2 * lax.rem(z, 2)
        if isinstance(i, int):
            return (z, near, 2 - hi, 3 - 3 * hi)[i]
        return jnp.where(i == 0, z, jnp.where(i == 1, near, jnp.where(i == 2, 2 - hi, 3 - 3 * hi)))

    def copy(self, send_kind, recv, i, t, r, s, dev):
        size = self.rows if s is None else self.rows // self.subs
        block = self.slots.at[t, r, pl.ds(0 if s is None else s * size, size)]
        return pltpu.make_async_remote_copy(
            src_ref=block, dst_ref=block, send_sem=self.sends.at[send_kind, i], recv_sem=recv, device_id=dev, device_id_type=MESH)

    def near(self, i, t, s=None):
        return self.copy(0, self.recvs.at[0, t, s or 0], i, t, self.p.r, s, self.p.near)

    def far(self, i, t, s=None):
        return self.copy(1, self.recvs.at[0, t, s or 0], i, t, self.p.r, s, self.p.far)

    def cross(self, i, t, s=None):
        return self.copy(2, self.recvs.at[1, t, s or 0], i, t, self.p.r, s, self.p.across_id)

    def mate(self, i, t, s=None):
        return self.copy(3, self.mate_recvs.at[0, t], i, t, self.p.r, s, self.p.mate_id)

    def mate_across(self, i, t, s=None):
        return self.copy(4, self.mate_recvs.at[1, t], i, t, self.p.across, s, self.p.mate_id)

    def start_line(self, s):
        self.near(0, self.p.z, s).start()

        @pl.when(self.p.inner)
        def _():
            self.far(0, self.p.z, s).start()

    def start_plane(self, s):
        self.cross(0, self.p.z, s).start()
        if self.mate_recvs is not None:
            self.mate(0, self.p.z, s).start()

    def step(self, i, s):
        t = self.order(i)
        self.near(i, t, s).wait_recv()

        @pl.when(self.p.inner)
        def _():
            @pl.when(i == 1)
            def _():
                self.far(i, t, s).start()

            @pl.when(i != 1)
            def _():
                self.near(i, t, s).start()

        self.cross(i, t, s).start()
        if self.mate_recvs is not None:
            self.mate(i, t, s).start()

    def pass_across(self, i, s):
        t = self.order(i)
        self.cross(i, t, s).wait_recv()
        if self.mate_recvs is not None:
            self.mate_across(i, t, s).start()

    def wait_same(self, i):
        self.mate(i, self.order(i)).wait_recv()

    def wait_across(self, i):
        self.mate_across(i, self.order(i)).wait_recv()

    def finish(self):
        self.near(0, self.p.z).wait_send()

        @pl.when(self.p.inner)
        def _():
            for i in range(4):
                (self.far if i < 2 else self.near)(i, self.order(i)).wait_send()

        for i in range(4):
            t = self.order(i)
            self.cross(i, t).wait_send()
            if self.mate_recvs is not None:
                self.mate(i, t).wait_send()
                self.mate_across(i, t).wait_send()


def slot_codes(mask_row):
    n = mask_row.shape[1]
    upper = (lax.broadcasted_iota(jnp.int32, (n, n), 0) <= lax.broadcasted_iota(jnp.int32, (n, n), 1)).astype(F32)
    mask_f = jnp.broadcast_to(mask_row.astype(F32), (8, n))
    rank = nn(mask_f, upper)[0:1]
    return jnp.where(mask_row == 1, rank - 1.0, float(SLOTS))


def one_hot(code_row, rows):
    ids = lax.broadcasted_iota(jnp.int32, (rows, code_row.shape[1]), 0).astype(F32)
    return (ids == code_row).astype(BF16)


def column(row):
    return jnp.transpose(jnp.broadcast_to(row, (BLK, row.shape[1])))


def attend(keys, vals, qtm, state):
    top_ref, tot_ref, acc_ref, sc_ref, pr_ref = state
    n = keys.shape[0]
    ones = jnp.ones((16, n), BF16)
    scale = 32 ** -0.5
    highs = []
    for pair in range(8):
        cols = slice(BLK * (pair // 2), BLK * (pair // 2) + BLK)
        sc = nn(keys[:, cols], qtm[pair])
        sc_ref[pair, 0:n] = sc
        highs.append(jnp.max(sc, axis=0, keepdims=True))
    keeps = []
    for pair in range(8):
        old = top_ref[pair:pair + 1, :]
        new = jnp.maximum(old, highs[pair])
        top_ref[pair:pair + 1, :] = new
        keeps.append(jnp.exp((old - new) * scale))
        pr_ref[pair, 0:n] = jnp.exp((sc_ref[pair, 0:n] - new) * scale).astype(BF16)
    for pair in range(8):
        o = nn(jnp.concatenate([vals[64 * pair:64 * pair + 64], ones], axis=0), pr_ref[pair, 0:n])
        keep = keeps[pair]
        tot_ref[pair:pair + 1, :] = tot_ref[pair:pair + 1, :] * keep + o[64:65]
        a, b = slice(64 * pair, 64 * pair + 32), slice(64 * pair + 32, 64 * pair + 64)
        acc_ref[a, :] = acc_ref[a, :] * keep[:, 0:BLK] + o[0:32, 0:BLK]
        acc_ref[b, :] = acc_ref[b, :] * keep[:, BLK:256] + o[32:64, BLK:256]


def dec_front(l, a, vec_ref, wqkv, qtm, vbias, top_ref, tot_ref, acc_ref):
    row = lambda i: vec_ref[i, l:l + 1, :]
    qt = (nt(wqkv[l, 0:D], a) + column(row(4))).astype(BF16)
    vbias[...] = column(row(5))
    qtm[...] = jnp.zeros((8, BLK, 256), BF16)
    for head in range(16):
        base = 32 * (head % 4)
        qtm[head // 2, base:base + 32, BLK * (head % 2):BLK * (head % 2) + BLK] = qt[32 * head:32 * head + 32]
    top_ref[...] = jnp.full((8, 256), -jnp.inf, F32)
    tot_ref[...] = jnp.zeros((8, 256), F32)
    acc_ref[...] = jnp.zeros((D, BLK), F32)


def dec_keys(l, a, wqkv, vbias):
    keys = nt(a, wqkv[l, D:1024]).astype(BF16)
    vals = (nt(wqkv[l, 1024:3 * D], a) + jnp.concatenate([vbias[...]] * (a.shape[0] // BLK), axis=1)).astype(BF16)
    return keys, vals


def dec_back(l, h, vec_ref, wo, w1, w2, tot_ref, acc_ref):
    row = lambda i: vec_ref[i, l:l + 1, :]
    parts = []
    for head in range(16):
        inv = 1.0 / tot_ref[head // 2:head // 2 + 1, BLK * (head % 2):BLK * (head % 2) + BLK]
        parts.append((acc_ref[32 * head:32 * head + 32, :] * inv).astype(BF16))
    att = jnp.concatenate(parts, axis=0)
    res = (h.astype(F32) + tn(att, wo[l]) + row(6)).astype(BF16)
    b = layer_norm(res, row(2), row(3)).astype(BF16)
    acc = res.astype(F32) + row(7)
    for j in range(4):
        cols = pl.ds(D * j, D)
        m = gelu(nn(b, w1[l, :, cols]) + row(8 + j)).astype(BF16)
        acc = acc + nn(m, w2[l, cols, :])
    return acc.astype(BF16)


def kernel(mask_hbm, patches_hbm, pos_hbm, dpos_hbm, b_embed_hbm, evec_hbm, efin_hbm, mtok_hbm, dvec_hbm, dfin_hbm,
           w_embed_hbm, ewqkv_hbm, ewo_hbm, ew1_hbm, ew2_hbm, wdec_hbm, dwqkv_hbm, dwo_hbm, dw1_hbm, dw2_hbm,
           out_ref,
           mask_ref, patches_ref, pos_ref, dpos_ref, b_embed_ref, evec_ref, efin_ref, mtok_ref, dvec_ref, dfin_ref,
           w_embed, ewqkv, ewo, ew1, ew2, wdec, dwqkv, dwo, dw1, dw2, wsem,
           e_buf, p1_buf, e2_buf, p2_buf, f_all, att, ek, ev, zall, xsem, tsem,
           dall, a_all, table, qtm, vbias, top_ref, tot_ref, acc_ref, sc_ref, pr_ref, s1, r1, m1, s2, r2, m2):
    p = Peers()
    p.greet()
    loads = {}
    state = (top_ref, tot_ref, acc_ref, sc_ref, pr_ref)
    plan = [("mask", mask_hbm, mask_ref), ("patches", patches_hbm, patches_ref), ("pos", pos_hbm, pos_ref), ("dpos", dpos_hbm, dpos_ref),
            ("bias", b_embed_hbm, b_embed_ref), ("embed", w_embed_hbm, w_embed),
            ("evec", evec_hbm, evec_ref), ("efin", efin_hbm, efin_ref), ("mtok", mtok_hbm, mtok_ref), ("dvec", dvec_hbm, dvec_ref), ("dfin", dfin_hbm, dfin_ref)]
    soon = [name for name, *_ in plan]
    for l in range(2):
        plan += [((n, l), src.at[l], dst.at[l]) for n, src, dst in (("eqkv", ewqkv_hbm, ewqkv), ("eo", ewo_hbm, ewo), ("e1", ew1_hbm, ew1), ("e2", ew2_hbm, ew2))]
    plan += [("dec", wdec_hbm, wdec)]
    for l in range(2):
        plan += [((n, l), src.at[l], dst.at[l]) for n, src, dst in (("dqkv", dwqkv_hbm, dwqkv), ("do", dwo_hbm, dwo), ("d1", dw1_hbm, dw1), ("d2", dw2_hbm, dw2))]
    for i, (name, src, dst) in enumerate(plan):
        loads[name] = pltpu.make_async_copy(src, dst, wsem.at[i])
    for name in soon:
        loads[name].start()
    loads["mask"].wait()
    code = slot_codes(mask_ref[...])
    for name in ("patches", "pos", "bias", "embed"):
        loads[name].wait()
    sel = one_hot(code, SLOTS)
    picked = nn(sel, patches_ref[...]).astype(BF16)
    pos = nn(sel, pos_ref[...])
    have = jnp.sum(sel.astype(F32), axis=1, keepdims=True)
    for name, *_ in plan[len(soon):]:
        loads[name].start()
    emb = nn(picked, w_embed[...]) + b_embed_ref[...].reshape(1, E) + pos
    e_buf[...] = jnp.where(have > 0.5, emb, 0.0).astype(BF16)
    for name in ("dpos", "evec", "efin", "mtok", "dvec", "dfin"):
        loads[name].wait()
    dall[p.z, p.r, 0:BLK, :] = dpos_ref[...]
    dall[p.z, p.r, BLK:CODE, :] = jnp.broadcast_to(jnp.concatenate([code, jnp.zeros((1, 384), F32)], axis=1), (CODE - BLK, D)).astype(BF16)
    p.barrier()
    mate, across = p.mate_id, p.across_id
    first = remote(e_buf, p1_buf, xsem, 0, mate)
    first.start()
    first.wait_recv()
    both = e_buf[...].astype(F32) + p1_buf[...].astype(F32)
    e2_buf[...] = both.astype(BF16).reshape(2, 32, E)
    second = remote(e2_buf.at[p.core], p2_buf, xsem, 1, across)
    second.start()
    second.wait_recv()
    f_all[p.z, p.core] = (e2_buf[p.core].astype(F32) + p2_buf[...].astype(F32)).astype(BF16)
    g1 = Gather(p, dall, s1, r1, m1, CODE, 1)

    def half_block(j, t):
        block = f_all.at[t, p.core]
        return pltpu.make_async_remote_copy(
            src_ref=block, dst_ref=block, send_sem=tsem.at[0, j], recv_sem=tsem.at[1, t],
            device_id={"time": g1.order(j), "region": p.r}, device_id_type=MESH)

    for j in (3, 2, 1):
        half_block(j, p.z).start()
    g1.start_line(0)
    g1.start_plane(0)
    for j in (1, 2, 3):
        half_block(j, g1.order(j)).wait_recv()
    for j in (1, 2, 3):
        half_block(j, p.z).wait_send()
    first.wait_send()
    second.wait_send()
    h = jnp.concatenate([f_all[t, p.core] for t in range(4)], axis=0)
    lane = lax.broadcasted_iota(jnp.int32, (BLK, BLK), 1)
    for l in range(2):
        row = lambda i: evec_ref[i, l:l + 1, :]
        a = layer_norm(h, row(0), row(1)).astype(BF16)
        loads["eqkv", l].wait()
        ek[l, 0] = nt(a, ewqkv[l, E:2 * E]).astype(BF16)
        to_mate = [remote(ek.at[l, 0], ek.at[l, 1], xsem, 2 + 2 * l, mate), remote(ev.at[l, 0], ev.at[l, 1], xsem, 3 + 2 * l, mate)]
        ev[l, 0] = (nt(a, ewqkv[l, 2 * E:3 * E]) + row(5)).astype(BF16)
        for c in to_mate:
            c.start()
        q = nt(a, ewqkv[l, 0:E]) + row(4)
        for c in to_mate:
            c.wait()
        for g in range(6):
            cols = slice(BLK * g, BLK * g + BLK)
            k = jnp.concatenate([ek[l, 0, :, cols], ek[l, 1, :, cols]], axis=0)
            v = jnp.concatenate([ev[l, 0, :, cols], ev[l, 1, :, cols]], axis=0)
            outs = []
            for s in range(2):
                qm = jnp.where((lane // 64) == s, q[:, cols], 0.0).astype(BF16)
                sc = nt(qm, k)
                top = jnp.max(sc, axis=-1, keepdims=True)
                pr = jnp.exp((sc - top) * 0.125)
                tot = jnp.sum(pr, axis=-1, keepdims=True)
                outs.append(nn(pr.astype(BF16), v) * (1.0 / tot))
            att[:, cols] = jnp.where(lane < 64, outs[0], outs[1]).astype(BF16)
        if l == 0:
            g1.step(1, 0)

            @pl.when(p.inner)
            def _():
                g1.step(2, 0)

            g1.pass_across(0, 0)
        else:
            @pl.when(p.inner)
            def _():
                g1.step(3, 0)

            @pl.when(jnp.logical_not(p.inner))
            def _():
                g1.step(2, 0)

            g1.pass_across(1, 0)
        loads["eo", l].wait()
        res = (h.astype(F32) + nn(att[...], ewo[l]) + row(6)).astype(BF16)
        b = layer_norm(res, row(2), row(3)).astype(BF16)
        acc = res.astype(F32) + row(7)
        loads["e1", l].wait()
        loads["e2", l].wait()
        for j in range(4):
            cols = pl.ds(E * j, E)
            m = gelu(nn(b, ew1[l, :, cols]) + row(8 + j)).astype(BF16)
            acc = acc + nn(m, ew2[l, cols, :])
        h = acc.astype(BF16)
    loads["dec"].wait()
    zf = layer_norm(h, efin_ref[0:1, :], efin_ref[1:2, :]).astype(BF16)
    zall[p.core] = nn(zf, wdec[...]).astype(BF16).reshape(4, 32, D)
    zcopy = remote(zall.at[p.core], zall.at[p.core], xsem, 6, mate)
    zcopy.start()
    table[:, SLOTS:ZROWS, :] = jnp.broadcast_to(mtok_ref[...].astype(F32).reshape(1, 1, D), (4, ZROWS - SLOTS, D)).astype(BF16)
    zcopy.wait()
    for half in range(2):
        table[:, 32 * half:32 * half + 32, :] = zall[half]
    def token_rows(code, t, dpos):
        return (tn(one_hot(code, ZROWS), table[t]) + dpos.astype(F32)).astype(BF16)

    h = token_rows(slot_codes(mask_ref[...]), p.z, dpos_ref[...])
    loads["dqkv", 0].wait()
    dec_front(0, layer_norm(h, dvec_ref[0, 0:1, :], dvec_ref[1, 0:1, :]).astype(BF16), dvec_ref, dwqkv, qtm, vbias, top_ref, tot_ref, acc_ref)

    @pl.when(jnp.logical_not(p.inner))
    def _():
        g1.step(3, 0)
    def norm_rows(t, r):
        u = token_rows(dall[t, r, BLK:CODE, 0:BLK].astype(F32)[0:1], t, dall[t, r, 0:BLK, :])
        return layer_norm(u, dvec_ref[0, 0:1, :], dvec_ref[1, 0:1, :]).astype(BF16)

    def first_layer(i, carry):
        t = g1.order(i)

        @pl.when((i == 1) | (i == 2))
        def _():
            g1.pass_across(i + 1, 0)

        g1.wait_same(i)
        g1.wait_across(i)
        a = jnp.concatenate([norm_rows(t, r) for r in range(4)], axis=0)
        keys, vals = dec_keys(0, a, dwqkv, vbias)
        attend(keys, vals, qtm, state)
        return carry
    lax.fori_loop(0, 4, first_layer, 0)
    for n in ("do", "d1", "d2"):
        loads[n, 0].wait()
    h = dec_back(0, h, dvec_ref, dwo, dw1, dw2, tot_ref, acc_ref)
    g1.finish()
    a_all[p.z, p.r] = layer_norm(h, dvec_ref[0, 1:2, :], dvec_ref[1, 1:2, :]).astype(BF16)
    g2 = Gather(p, a_all, s2, r2, m2, BLK, SUBS)
    for s in range(SUBS):
        g2.start_line(s)
        g2.start_plane(s)
    loads["dqkv", 1].wait()
    dec_front(1, a_all[p.z, p.r], dvec_ref, dwqkv, qtm, vbias, top_ref, tot_ref, acc_ref)
    def chunk(i, half):
        t = g2.order(i)
        ra = lax.rem(p.r + 2 * half, 4)
        rb = lax.rem(p.mate + 2 * half, 4)
        keys, vals = dec_keys(1, jnp.concatenate([a_all[t, ra], a_all[t, rb]], axis=0), dwqkv, vbias)
        attend(keys, vals, qtm, state)

    def outer_step(i, s):
        @pl.when(jnp.logical_not(p.inner))
        def _():
            g2.step(i, s)

    def inner_step(i, s):
        @pl.when(p.inner)
        def _():
            g2.step(i, s)
    g2.wait_same(0)
    chunk(0, 0)
    for s in range(SUBS):
        g2.step(1, s)
        inner_step(2, s)
        g2.pass_across(0, s)
    for s in range(SUBS):
        inner_step(3, s)
    g2.wait_across(0)
    chunk(0, 1)
    for s in range(SUBS):
        outer_step(2, s)
    g2.wait_same(1)
    chunk(1, 0)
    for s in range(SUBS):
        g2.pass_across(1, s)
    g2.wait_same(2)
    chunk(2, 0)
    for s in range(SUBS):
        outer_step(3, s)
    g2.wait_across(1)
    chunk(1, 1)
    for s in range(SUBS):
        g2.pass_across(2, s)
    g2.wait_same(3)
    chunk(3, 0)
    g2.wait_across(2)
    chunk(2, 1)
    for s in range(SUBS):
        g2.pass_across(3, s)
    g2.wait_across(3)
    chunk(3, 1)
    for n in ("do", "d1", "d2"):
        loads[n, 1].wait()
    h = dec_back(1, h, dvec_ref, dwo, dw1, dw2, tot_ref, acc_ref)
    out_ref[...] = layer_norm(h, dfin_ref[0:1, :], dfin_ref[1:2, :]).astype(BF16)
    g2.finish()


VM = pl.BlockSpec(memory_space=pltpu.VMEM)
ANY = pl.BlockSpec(memory_space=pl.ANY)
DMA = pltpu.SemaphoreType.DMA


def solution(mesh):
    def local_step(patches, enc_pos, vis_mask, dec_pos, w_embed, b_embed, enc_vec, enc_wqkv, enc_wo, enc_w1, enc_w2, enc_final, w_dec_in, mask_token, dec_vec, dec_wqkv, dec_wo, dec_w1, dec_w2, dec_final, w_out):
        mask_row = vis_mask.reshape(1, BLK)
        wq_e = jnp.transpose(enc_wqkv, (0, 2, 3, 4, 1)).reshape(2, 3 * E, E)
        wq_d = jnp.transpose(dec_wqkv, (0, 2, 3, 4, 1)).reshape(2, 3 * D, D)
        wo_e = enc_wo.reshape(2, E, E)
        wo_d = dec_wo.reshape(2, D, D)
        vm = lambda *shape: pltpu.VMEM(shape, BF16)
        vf = lambda *shape: pltpu.VMEM(shape, F32)
        y = pl.pallas_call(
            kernel,
            out_shape=pltpu.VMEM((BLK, D), BF16),
            in_specs=[ANY] * 20,
            out_specs=VM,
            scratch_shapes=[
                pltpu.VMEM((1, BLK), jnp.int32), vm(BLK, E), vm(BLK, E), vm(BLK, D), vf(E), vf(12, 2, E), vf(2, E), vm(D), vf(12, 2, D), vf(2, D),
                vm(E, E), vm(2, 3 * E, E), vm(2, E, E), vm(2, E, 4 * E), vm(2, 4 * E, E), vm(E, D),
                vm(2, 3 * D, D), vm(2, D, D), vm(2, D, 4 * D), vm(2, 4 * D, D), DMA((28,)),
                vm(64, E), vm(64, E), vm(2, 32, E), vm(32, E), vm(4, 2, 32, E), vm(BLK, E), vm(2, 2, BLK, E), vm(2, 2, BLK, E), vm(2, 4, 32, D), DMA((2, 7)), DMA((2, 4)),
                vm(4, 4, CODE, D), vm(4, 4, BLK, D), vm(4, ZROWS, D), vm(8, BLK, 256), vf(D, BLK), vf(8, 256), vf(8, 256), vf(D, BLK), vf(8, D, 256), vm(8, D, 256),
                *Gather.sems(1, True), *Gather.sems(SUBS, True),
            ],
            compiler_params=pltpu.CompilerParams(collective_id=0, has_side_effects=True, vmem_limit_bytes=61 * 1024 * 1024),
            name="mae",
        )(mask_row, patches, enc_pos, dec_pos, b_embed, jnp.transpose(enc_vec, (1, 0, 2)), enc_final,
          mask_token, jnp.transpose(dec_vec, (1, 0, 2)), dec_final,
          w_embed, wq_e, wo_e, enc_w1, enc_w2, w_dec_in, wq_d, wo_d, dec_w1, dec_w2)
        return jnp.dot(y, w_out, preferred_element_type=F32)

    token_rows = P(TOKEN_AXES, None)
    token_flags = P(TOKEN_AXES)
    replicated = P()
    in_specs = (token_rows, token_rows, token_flags, token_rows) + (replicated,) * 17
    return jax.shard_map(local_step, mesh=mesh, in_specs=in_specs, out_specs=token_rows, check_vma=False)
```

```python
import functools
import jax
import jax.numpy as jnp
from jax import lax
from jax.experimental import pallas as pl
from jax.experimental.pallas import tpu as pltpu
from jax.sharding import PartitionSpec as P

LN_EPS = 1e-6
TOKEN_AXES = ("batch", "time", "region")
MESH = pl.DeviceIdType.MESH
F32 = jnp.float32
BF16 = jnp.bfloat16
BLK = 128
CODE = 144
E = 768
D = 512
PART = 16
SLOTS = 64
SUBS = 4
ZROWS = 128


def nn(a, b):
    return jnp.dot(a, b, preferred_element_type=F32)


def nt(a, b):
    return lax.dot_general(a, b, (((1,), (1,)), ((), ())), preferred_element_type=F32)


def tn(a, b):
    return lax.dot_general(a, b, (((0,), (0,)), ((), ())), preferred_element_type=F32)


def layer_norm(hidden, gain, shift):
    hid = hidden.astype(F32)
    mean = jnp.mean(hid, axis=-1, keepdims=True)
    centered = hid - mean
    var = jnp.mean(centered * centered, axis=-1, keepdims=True)
    return centered * lax.rsqrt(var + LN_EPS) * gain + shift


def gelu(x):
    return 0.5 * x * (1.0 + lax.erf(x * 0.7071067811865476))


class Peers:
    def __init__(self):
        self.z = lax.axis_index("time")
        self.r = lax.axis_index("region")
        self.core = lax.rem(self.r, 2)
        self.mate = self.r + 1 - 2 * self.core
        self.row = self.r // 2
        self.across = lax.rem(self.r + 2, 4)
        self.inner = (self.z == 1) | (self.z == 2)
        self.mate_id = {"time": self.z, "region": self.mate}
        self.across_id = {"time": self.z, "region": self.across}
        self.near = {"time": self.z + 1 - 2 * lax.rem(self.z, 2), "region": self.r}
        self.far = {"time": 3 - self.z, "region": self.r}

    def zth(self, k):
        return lax.rem(self.z + k, 4)

    def ids(self):
        out = [{"time": self.z, "region": self.mate}, {"time": self.z, "region": self.across}]
        return out + [{"time": self.zth(k), "region": self.r} for k in (1, 2, 3)]

    def greet(self):
        for dev in self.ids():
            pl.semaphore_signal(pltpu.get_barrier_semaphore(), inc=1, device_id=dev, device_id_type=MESH)

    def barrier(self):
        pl.semaphore_wait(pltpu.get_barrier_semaphore(), 5)


def remote(src, dst, sems, i, dev):
    return pltpu.make_async_remote_copy(
        src_ref=src, dst_ref=dst, send_sem=sems.at[0, i], recv_sem=sems.at[1, i],
        device_id=dev, device_id_type=MESH)


class Gather:
    def __init__(self, peers, slots, sends, recvs, mate_recvs, rows, subs):
        self.p, self.slots, self.sends, self.recvs, self.mate_recvs = peers, slots, sends, recvs, mate_recvs
        self.rows, self.subs = rows, subs

    @staticmethod
    def sems(subs, mates):
        return [DMA((5 if mates else 3, 4)), DMA((2, 4, subs)), DMA((2, 4))][:3 if mates else 2]

    def order(self, i):
        z = self.p.z
        hi = z // 2
        near = z + 1 - 2 * lax.rem(z, 2)
        if isinstance(i, int):
            return (z, near, 2 - hi, 3 - 3 * hi)[i]
        return jnp.where(i == 0, z, jnp.where(i == 1, near, jnp.where(i == 2, 2 - hi, 3 - 3 * hi)))

    def copy(self, send_kind, recv, i, t, r, s, dev):
        size = self.rows if s is None else self.rows // self.subs
        block = self.slots.at[t, r, pl.ds(0 if s is None else s * size, size)]
        return pltpu.make_async_remote_copy(
            src_ref=block, dst_ref=block, send_sem=self.sends.at[send_kind, i], recv_sem=recv, device_id=dev, device_id_type=MESH)

    def near(self, i, t, s=None):
        return self.copy(0, self.recvs.at[0, t, s or 0], i, t, self.p.r, s, self.p.near)

    def far(self, i, t, s=None):
        return self.copy(1, self.recvs.at[0, t, s or 0], i, t, self.p.r, s, self.p.far)

    def cross(self, i, t, s=None):
        return self.copy(2, self.recvs.at[1, t, s or 0], i, t, self.p.r, s, self.p.across_id)

    def mate(self, i, t, s=None):
        return self.copy(3, self.mate_recvs.at[0, t], i, t, self.p.r, s, self.p.mate_id)

    def mate_across(self, i, t, s=None):
        return self.copy(4, self.mate_recvs.at[1, t], i, t, self.p.across, s, self.p.mate_id)

    def start_line(self, s):
        self.near(0, self.p.z, s).start()

        @pl.when(self.p.inner)
        def _():
            self.far(0, self.p.z, s).start()

    def start_plane(self, s):
        self.cross(0, self.p.z, s).start()
        if self.mate_recvs is not None:
            self.mate(0, self.p.z, s).start()

    def step(self, i, s):
        t = self.order(i)
        self.near(i, t, s).wait_recv()

        @pl.when(self.p.inner)
        def _():
            @pl.when(i == 1)
            def _():
                self.far(i, t, s).start()

            @pl.when(i != 1)
            def _():
                self.near(i, t, s).start()

        self.cross(i, t, s).start()
        if self.mate_recvs is not None:
            self.mate(i, t, s).start()

    def pass_across(self, i, s):
        t = self.order(i)
        self.cross(i, t, s).wait_recv()
        if self.mate_recvs is not None:
            self.mate_across(i, t, s).start()

    def wait_same(self, i):
        self.mate(i, self.order(i)).wait_recv()

    def wait_across(self, i):
        self.mate_across(i, self.order(i)).wait_recv()

    def finish(self):
        self.near(0, self.p.z).wait_send()

        @pl.when(self.p.inner)
        def _():
            for i in range(4):
                (self.far if i < 2 else self.near)(i, self.order(i)).wait_send()

        for i in range(4):
            t = self.order(i)
            self.cross(i, t).wait_send()
            if self.mate_recvs is not None:
                self.mate(i, t).wait_send()
                self.mate_across(i, t).wait_send()


def slot_codes(mask_row):
    n = mask_row.shape[1]
    upper = (lax.broadcasted_iota(jnp.int32, (n, n), 0) <= lax.broadcasted_iota(jnp.int32, (n, n), 1)).astype(F32)
    mask_f = jnp.broadcast_to(mask_row.astype(F32), (8, n))
    rank = nn(mask_f, upper)[0:1]
    return jnp.where(mask_row == 1, rank - 1.0, float(SLOTS))


def one_hot(code_row, rows):
    ids = lax.broadcasted_iota(jnp.int32, (rows, code_row.shape[1]), 0).astype(F32)
    return (ids == code_row).astype(BF16)


def column(row):
    return jnp.transpose(jnp.broadcast_to(row, (BLK, row.shape[1])))


def attend(keys, vals, qtm, state):
    top_ref, tot_ref, acc_ref, sc_ref, pr_ref = state
    n = keys.shape[0]
    ones = jnp.ones((16, n), BF16)
    scale = 32 ** -0.5
    highs = []
    for pair in range(8):
        cols = slice(BLK * (pair // 2), BLK * (pair // 2) + BLK)
        sc = nn(keys[:, cols], qtm[pair])
        sc_ref[pair, 0:n] = sc
        highs.append(jnp.max(sc, axis=0, keepdims=True))
    keeps = []
    for pair in range(8):
        old = top_ref[pair:pair + 1, :]
        new = jnp.maximum(old, highs[pair])
        top_ref[pair:pair + 1, :] = new
        keeps.append(jnp.exp((old - new) * scale))
        pr_ref[pair, 0:n] = jnp.exp((sc_ref[pair, 0:n] - new) * scale).astype(BF16)
    for pair in range(8):
        o = nn(jnp.concatenate([vals[64 * pair:64 * pair + 64], ones], axis=0), pr_ref[pair, 0:n])
        keep = keeps[pair]
        tot_ref[pair:pair + 1, :] = tot_ref[pair:pair + 1, :] * keep + o[64:65]
        a, b = slice(64 * pair, 64 * pair + 32), slice(64 * pair + 32, 64 * pair + 64)
        acc_ref[a, :] = acc_ref[a, :] * keep[:, 0:BLK] + o[0:32, 0:BLK]
        acc_ref[b, :] = acc_ref[b, :] * keep[:, BLK:256] + o[32:64, BLK:256]


def dec_front(l, a, vec_ref, wqkv, qtm, vbias, top_ref, tot_ref, acc_ref):
    row = lambda i: vec_ref[i, l:l + 1, :]
    qt = (nt(wqkv[l, 0:D], a) + column(row(4))).astype(BF16)
    vbias[...] = column(row(5))
    qtm[...] = jnp.zeros((8, BLK, 256), BF16)
    for head in range(16):
        base = 32 * (head % 4)
        qtm[head // 2, base:base + 32, BLK * (head % 2):BLK * (head % 2) + BLK] = qt[32 * head:32 * head + 32]
    top_ref[...] = jnp.full((8, 256), -jnp.inf, F32)
    tot_ref[...] = jnp.zeros((8, 256), F32)
    acc_ref[...] = jnp.zeros((D, BLK), F32)


def dec_keys(l, a, wqkv, vbias):
    keys = nt(a, wqkv[l, D:1024]).astype(BF16)
    vals = (nt(wqkv[l, 1024:3 * D], a) + jnp.concatenate([vbias[...]] * (a.shape[0] // BLK), axis=1)).astype(BF16)
    return keys, vals


def dec_back(l, h, vec_ref, wo, w1, w2, tot_ref, acc_ref):
    row = lambda i: vec_ref[i, l:l + 1, :]
    parts = []
    for head in range(16):
        inv = 1.0 / tot_ref[head // 2:head // 2 + 1, BLK * (head % 2):BLK * (head % 2) + BLK]
        parts.append((acc_ref[32 * head:32 * head + 32, :] * inv).astype(BF16))
    att = jnp.concatenate(parts, axis=0)
    res = (h.astype(F32) + tn(att, wo[l]) + row(6)).astype(BF16)
    b = layer_norm(res, row(2), row(3)).astype(BF16)
    acc = res.astype(F32) + row(7)
    for j in range(4):
        cols = pl.ds(D * j, D)
        m = gelu(nn(b, w1[l, :, cols]) + row(8 + j)).astype(BF16)
        acc = acc + nn(m, w2[l, cols, :])
    return acc.astype(BF16)


def kernel(mask_hbm, patches_hbm, pos_hbm, dpos_hbm, b_embed_hbm, evec_hbm, efin_hbm, mtok_hbm, dvec_hbm, dfin_hbm,
           w_embed_hbm, ewqkv_hbm, ewo_hbm, ew1_hbm, ew2_hbm, wdec_hbm, dwqkv_hbm, dwo_hbm, dw1_hbm, dw2_hbm,
           out_ref,
           mask_ref, patches_ref, pos_ref, dpos_ref, b_embed_ref, evec_ref, efin_ref, mtok_ref, dvec_ref, dfin_ref,
           w_embed, ewqkv, ewo, ew1, ew2, wdec, dwqkv, dwo, dw1, dw2, wsem,
           e_buf, p1_buf, e2_buf, p2_buf, f_all, att, ek, ev, zall, xsem, tsem, usem,
           dall, a_all, table, qtm, vbias, top_ref, tot_ref, acc_ref, sc_ref, pr_ref, s1, r1, m1, s2, r2, m2):
    p = Peers()
    p.greet()
    loads = {}
    state = (top_ref, tot_ref, acc_ref, sc_ref, pr_ref)
    plan = [("mask", mask_hbm, mask_ref), ("patches", patches_hbm, patches_ref), ("pos", pos_hbm, pos_ref), ("dpos", dpos_hbm, dpos_ref),
            ("bias", b_embed_hbm, b_embed_ref), ("embed", w_embed_hbm, w_embed),
            ("evec", evec_hbm, evec_ref), ("efin", efin_hbm, efin_ref), ("mtok", mtok_hbm, mtok_ref), ("dvec", dvec_hbm, dvec_ref), ("dfin", dfin_hbm, dfin_ref)]
    soon = [name for name, *_ in plan]
    for l in range(2):
        plan += [((n, l), src.at[l], dst.at[l]) for n, src, dst in (("eqkv", ewqkv_hbm, ewqkv), ("eo", ewo_hbm, ewo), ("e1", ew1_hbm, ew1), ("e2", ew2_hbm, ew2))]
    plan += [("dec", wdec_hbm, wdec)]
    for l in range(2):
        plan += [((n, l), src.at[l], dst.at[l]) for n, src, dst in (("dqkv", dwqkv_hbm, dwqkv), ("do", dwo_hbm, dwo), ("d1", dw1_hbm, dw1), ("d2", dw2_hbm, dw2))]
    for i, (name, src, dst) in enumerate(plan):
        loads[name] = pltpu.make_async_copy(src, dst, wsem.at[i])
    for name in soon:
        loads[name].start()
    loads["mask"].wait()
    code = slot_codes(mask_ref[...])
    sel = one_hot(code, SLOTS)
    have = jnp.sum(sel.astype(F32), axis=1, keepdims=True)
    loads["patches"].wait()
    picked = nn(sel, patches_ref[...]).astype(BF16)
    loads["pos"].wait()
    pos = nn(sel, pos_ref[...])
    loads["bias"].wait()
    loads["embed"].wait()
    for name, *_ in plan[len(soon):]:
        loads[name].start()
    emb = nn(picked, w_embed[...]) + b_embed_ref[...].reshape(1, E) + pos
    e_buf[...] = jnp.where(have > 0.5, emb, 0.0).astype(BF16)
    for name in ("dpos", "evec", "efin", "mtok", "dvec", "dfin"):
        loads[name].wait()
    dall[p.z, p.r, 0:BLK, :] = dpos_ref[...]
    dall[p.z, p.r, BLK:CODE, :] = jnp.broadcast_to(jnp.concatenate([code, jnp.zeros((1, 384), F32)], axis=1), (CODE - BLK, D)).astype(BF16)
    p.barrier()
    mate, across = p.mate_id, p.across_id
    first = remote(e_buf, p1_buf, xsem, 0, mate)
    first.start()
    first.wait_recv()
    both = e_buf[...].astype(F32) + p1_buf[...].astype(F32)
    e2_buf[...] = both.astype(BF16).reshape(2, 32, E)
    def part(s):
        return pl.ds(PART * s, PART)

    g1 = Gather(p, dall, s1, r1, m1, CODE, 1)
    second = [
        pltpu.make_async_remote_copy(
            src_ref=e2_buf.at[p.core, part(s)], dst_ref=p2_buf.at[part(s)], send_sem=usem.at[0, s], recv_sem=usem.at[1, s],
            device_id=across, device_id_type=MESH) for s in (0, 1)]
    for c in second:
        c.start()

    def half_block(j, t, s):
        block = f_all.at[t, p.core, part(s)]
        return pltpu.make_async_remote_copy(
            src_ref=block, dst_ref=block, send_sem=tsem.at[0, j, s], recv_sem=tsem.at[1, t, s],
            device_id={"time": g1.order(j), "region": p.r}, device_id_type=MESH)

    for s in (0, 1):
        second[s].wait_recv()
        f_all[p.z, p.core, part(s)] = (e2_buf[p.core, part(s)].astype(F32) + p2_buf[part(s)].astype(F32)).astype(BF16)
        for j in (3, 2, 1):
            half_block(j, p.z, s).start()
    g1.start_line(0)
    g1.start_plane(0)
    first.wait_send()
    for s in (0, 1):
        second[s].wait_send()
        for j in (1, 2, 3):
            half_block(j, g1.order(j), s).wait_recv()
            half_block(j, p.z, s).wait_send()
    h = jnp.concatenate([f_all[t, p.core] for t in range(4)], axis=0)
    lane = lax.broadcasted_iota(jnp.int32, (BLK, BLK), 1)
    for l in range(2):
        row = lambda i: evec_ref[i, l:l + 1, :]
        a = layer_norm(h, row(0), row(1)).astype(BF16)
        loads["eqkv", l].wait()
        ek[l, 0] = nt(a, ewqkv[l, E:2 * E]).astype(BF16)
        to_mate = [remote(ek.at[l, 0], ek.at[l, 1], xsem, 2 + 2 * l, mate), remote(ev.at[l, 0], ev.at[l, 1], xsem, 3 + 2 * l, mate)]
        ev[l, 0] = (nt(a, ewqkv[l, 2 * E:3 * E]) + row(5)).astype(BF16)
        for c in to_mate:
            c.start()
        q = nt(a, ewqkv[l, 0:E]) + row(4)
        for c in to_mate:
            c.wait()
        for g in range(6):
            cols = slice(BLK * g, BLK * g + BLK)
            k = jnp.concatenate([ek[l, 0, :, cols], ek[l, 1, :, cols]], axis=0)
            v = jnp.concatenate([ev[l, 0, :, cols], ev[l, 1, :, cols]], axis=0)
            outs = []
            for s in range(2):
                qm = jnp.where((lane // 64) == s, q[:, cols], 0.0).astype(BF16)
                sc = nt(qm, k)
                top = jnp.max(sc, axis=-1, keepdims=True)
                pr = jnp.exp((sc - top) * 0.125)
                tot = jnp.sum(pr, axis=-1, keepdims=True)
                outs.append(nn(pr.astype(BF16), v) * (1.0 / tot))
            att[:, cols] = jnp.where(lane < 64, outs[0], outs[1]).astype(BF16)
        if l == 0:
            g1.step(1, 0)

            @pl.when(p.inner)
            def _():
                g1.step(2, 0)

            g1.pass_across(0, 0)
        else:
            @pl.when(p.inner)
            def _():
                g1.step(3, 0)

            @pl.when(jnp.logical_not(p.inner))
            def _():
                g1.step(2, 0)

            g1.pass_across(1, 0)
        loads["eo", l].wait()
        res = (h.astype(F32) + nn(att[...], ewo[l]) + row(6)).astype(BF16)
        b = layer_norm(res, row(2), row(3)).astype(BF16)
        acc = res.astype(F32) + row(7)
        loads["e1", l].wait()
        loads["e2", l].wait()
        for j in range(4):
            cols = pl.ds(E * j, E)
            m = gelu(nn(b, ew1[l, :, cols]) + row(8 + j)).astype(BF16)
            acc = acc + nn(m, ew2[l, cols, :])
        h = acc.astype(BF16)
    loads["dec"].wait()
    zf = layer_norm(h, efin_ref[0:1, :], efin_ref[1:2, :]).astype(BF16)
    zall[p.core] = nn(zf, wdec[...]).astype(BF16).reshape(4, 32, D)
    zcopy = remote(zall.at[p.core], zall.at[p.core], xsem, 6, mate)
    zcopy.start()
    table[:, SLOTS:ZROWS, :] = jnp.broadcast_to(mtok_ref[...].astype(F32).reshape(1, 1, D), (4, ZROWS - SLOTS, D)).astype(BF16)
    zcopy.wait()
    for half in range(2):
        table[:, 32 * half:32 * half + 32, :] = zall[half]
    def token_rows(code, t, dpos):
        return (tn(one_hot(code, ZROWS), table[t]) + dpos.astype(F32)).astype(BF16)

    h = token_rows(slot_codes(mask_ref[...]), p.z, dpos_ref[...])
    loads["dqkv", 0].wait()
    dec_front(0, layer_norm(h, dvec_ref[0, 0:1, :], dvec_ref[1, 0:1, :]).astype(BF16), dvec_ref, dwqkv, qtm, vbias, top_ref, tot_ref, acc_ref)

    @pl.when(jnp.logical_not(p.inner))
    def _():
        g1.step(3, 0)
    def norm_rows(t, r):
        u = token_rows(dall[t, r, BLK:CODE, 0:BLK].astype(F32)[0:1], t, dall[t, r, 0:BLK, :])
        return layer_norm(u, dvec_ref[0, 0:1, :], dvec_ref[1, 0:1, :]).astype(BF16)

    def first_layer(i, carry):
        t = g1.order(i)

        @pl.when((i == 1) | (i == 2))
        def _():
            g1.pass_across(i + 1, 0)

        g1.wait_same(i)
        g1.wait_across(i)
        a = jnp.concatenate([norm_rows(t, r) for r in range(4)], axis=0)
        keys, vals = dec_keys(0, a, dwqkv, vbias)
        attend(keys, vals, qtm, state)
        return carry
    lax.fori_loop(0, 4, first_layer, 0)
    for n in ("do", "d1", "d2"):
        loads[n, 0].wait()
    h = dec_back(0, h, dvec_ref, dwo, dw1, dw2, tot_ref, acc_ref)
    g1.finish()
    a_all[p.z, p.r] = layer_norm(h, dvec_ref[0, 1:2, :], dvec_ref[1, 1:2, :]).astype(BF16)
    g2 = Gather(p, a_all, s2, r2, m2, BLK, SUBS)
    for s in range(SUBS):
        g2.start_line(s)
        g2.start_plane(s)
    loads["dqkv", 1].wait()
    dec_front(1, a_all[p.z, p.r], dvec_ref, dwqkv, qtm, vbias, top_ref, tot_ref, acc_ref)
    def chunk(i, half):
        t = g2.order(i)
        ra = lax.rem(p.r + 2 * half, 4)
        rb = lax.rem(p.mate + 2 * half, 4)
        keys, vals = dec_keys(1, jnp.concatenate([a_all[t, ra], a_all[t, rb]], axis=0), dwqkv, vbias)
        attend(keys, vals, qtm, state)

    def outer_step(i, s):
        @pl.when(jnp.logical_not(p.inner))
        def _():
            g2.step(i, s)

    def inner_step(i, s):
        @pl.when(p.inner)
        def _():
            g2.step(i, s)
    g2.wait_same(0)
    chunk(0, 0)
    for s in range(SUBS):
        g2.step(1, s)
        inner_step(2, s)
        g2.pass_across(0, s)
    for s in range(SUBS):
        inner_step(3, s)
    g2.wait_across(0)
    chunk(0, 1)
    for s in range(SUBS):
        outer_step(2, s)
    g2.wait_same(1)
    chunk(1, 0)
    for s in range(SUBS):
        g2.pass_across(1, s)
    g2.wait_same(2)
    chunk(2, 0)
    for s in range(SUBS):
        outer_step(3, s)
    g2.wait_across(1)
    chunk(1, 1)
    for s in range(SUBS):
        g2.pass_across(2, s)
    g2.wait_same(3)
    chunk(3, 0)
    g2.wait_across(2)
    chunk(2, 1)
    for s in range(SUBS):
        g2.pass_across(3, s)
    g2.wait_across(3)
    chunk(3, 1)
    for n in ("do", "d1", "d2"):
        loads[n, 1].wait()
    h = dec_back(1, h, dvec_ref, dwo, dw1, dw2, tot_ref, acc_ref)
    out_ref[...] = layer_norm(h, dfin_ref[0:1, :], dfin_ref[1:2, :]).astype(BF16)
    g2.finish()


VM = pl.BlockSpec(memory_space=pltpu.VMEM)
ANY = pl.BlockSpec(memory_space=pl.ANY)
DMA = pltpu.SemaphoreType.DMA


def solution(mesh):
    def local_step(patches, enc_pos, vis_mask, dec_pos, w_embed, b_embed, enc_vec, enc_wqkv, enc_wo, enc_w1, enc_w2, enc_final, w_dec_in, mask_token, dec_vec, dec_wqkv, dec_wo, dec_w1, dec_w2, dec_final, w_out):
        mask_row = vis_mask.reshape(1, BLK)
        wq_e = jnp.transpose(enc_wqkv, (0, 2, 3, 4, 1)).reshape(2, 3 * E, E)
        wq_d = jnp.transpose(dec_wqkv, (0, 2, 3, 4, 1)).reshape(2, 3 * D, D)
        wo_e = enc_wo.reshape(2, E, E)
        wo_d = dec_wo.reshape(2, D, D)
        vm = lambda *shape: pltpu.VMEM(shape, BF16)
        vf = lambda *shape: pltpu.VMEM(shape, F32)
        y = pl.pallas_call(
            kernel,
            out_shape=pltpu.VMEM((BLK, D), BF16),
            in_specs=[ANY] * 20,
            out_specs=VM,
            scratch_shapes=[
                pltpu.VMEM((1, BLK), jnp.int32), vm(BLK, E), vm(BLK, E), vm(BLK, D), vf(E), vf(12, 2, E), vf(2, E), vm(D), vf(12, 2, D), vf(2, D),
                vm(E, E), vm(2, 3 * E, E), vm(2, E, E), vm(2, E, 4 * E), vm(2, 4 * E, E), vm(E, D),
                vm(2, 3 * D, D), vm(2, D, D), vm(2, D, 4 * D), vm(2, 4 * D, D), DMA((28,)),
                vm(64, E), vm(64, E), vm(2, 32, E), vm(32, E), vm(4, 2, 32, E), vm(BLK, E), vm(2, 2, BLK, E), vm(2, 2, BLK, E), vm(2, 4, 32, D), DMA((2, 7)), DMA((2, 4, 2)), DMA((2, 2)),
                vm(4, 4, CODE, D), vm(4, 4, BLK, D), vm(4, ZROWS, D), vm(8, BLK, 256), vf(D, BLK), vf(8, 256), vf(8, 256), vf(D, BLK), vf(8, D, 256), vm(8, D, 256),
                *Gather.sems(1, True), *Gather.sems(SUBS, True),
            ],
            compiler_params=pltpu.CompilerParams(collective_id=0, has_side_effects=True, vmem_limit_bytes=61 * 1024 * 1024),
            name="mae",
        )(mask_row, patches, enc_pos, dec_pos, b_embed, jnp.transpose(enc_vec, (1, 0, 2)), enc_final,
          mask_token, jnp.transpose(dec_vec, (1, 0, 2)), dec_final,
          w_embed, wq_e, wo_e, enc_w1, enc_w2, w_dec_in, wq_d, wo_d, dec_w1, dec_w2)
        return jnp.dot(y, w_out, preferred_element_type=F32)

    token_rows = P(TOKEN_AXES, None)
    token_flags = P(TOKEN_AXES)
    replicated = P()
    in_specs = (token_rows, token_rows, token_flags, token_rows) + (replicated,) * 17
    return jax.shard_map(local_step, mesh=mesh, in_specs=in_specs, out_specs=token_rows, check_vma=False)
```

```python
import functools
import jax
import jax.numpy as jnp
from jax import lax
from jax.experimental import pallas as pl
from jax.experimental.pallas import tpu as pltpu
from jax.sharding import PartitionSpec as P

LN_EPS = 1e-6
TOKEN_AXES = ("batch", "time", "region")
MESH = pl.DeviceIdType.MESH
F32 = jnp.float32
BF16 = jnp.bfloat16
BLK = 128
CODE = 144
E = 768
D = 512
PART = 16
SLOTS = 64
SUBS = 4
ZROWS = 128


def nn(a, b):
    return jnp.dot(a, b, preferred_element_type=F32)


def nt(a, b):
    return lax.dot_general(a, b, (((1,), (1,)), ((), ())), preferred_element_type=F32)


def tn(a, b):
    return lax.dot_general(a, b, (((0,), (0,)), ((), ())), preferred_element_type=F32)


def layer_norm(hidden, gain, shift):
    hid = hidden.astype(F32)
    mean = jnp.mean(hid, axis=-1, keepdims=True)
    centered = hid - mean
    var = jnp.mean(centered * centered, axis=-1, keepdims=True)
    return centered * lax.rsqrt(var + LN_EPS) * gain + shift


def gelu(x):
    return 0.5 * x * (1.0 + lax.erf(x * 0.7071067811865476))


class Peers:
    def __init__(self):
        self.z = lax.axis_index("time")
        self.r = lax.axis_index("region")
        self.core = lax.rem(self.r, 2)
        self.mate = self.r + 1 - 2 * self.core
        self.row = self.r // 2
        self.across = lax.rem(self.r + 2, 4)
        self.inner = (self.z == 1) | (self.z == 2)
        self.mate_id = {"time": self.z, "region": self.mate}
        self.across_id = {"time": self.z, "region": self.across}
        self.near = {"time": self.z + 1 - 2 * lax.rem(self.z, 2), "region": self.r}
        self.far = {"time": 3 - self.z, "region": self.r}

    def zth(self, k):
        return lax.rem(self.z + k, 4)

    def ids(self):
        out = [{"time": self.z, "region": self.mate}, {"time": self.z, "region": self.across}]
        return out + [{"time": self.zth(k), "region": self.r} for k in (1, 2, 3)]

    def greet(self):
        for dev in self.ids():
            pl.semaphore_signal(pltpu.get_barrier_semaphore(), inc=1, device_id=dev, device_id_type=MESH)

    def barrier(self):
        pl.semaphore_wait(pltpu.get_barrier_semaphore(), 5)


def remote(src, dst, sems, i, dev):
    return pltpu.make_async_remote_copy(
        src_ref=src, dst_ref=dst, send_sem=sems.at[0, i], recv_sem=sems.at[1, i],
        device_id=dev, device_id_type=MESH)


class Gather:
    def __init__(self, peers, slots, sends, recvs, mate_recvs, rows, subs):
        self.p, self.slots, self.sends, self.recvs, self.mate_recvs = peers, slots, sends, recvs, mate_recvs
        self.rows, self.subs = rows, subs

    @staticmethod
    def sems(subs, mates):
        return [DMA((5 if mates else 3, 4)), DMA((2, 4, subs)), DMA((2, 4))][:3 if mates else 2]

    def order(self, i):
        z = self.p.z
        hi = z // 2
        near = z + 1 - 2 * lax.rem(z, 2)
        if isinstance(i, int):
            return (z, near, 2 - hi, 3 - 3 * hi)[i]
        return jnp.where(i == 0, z, jnp.where(i == 1, near, jnp.where(i == 2, 2 - hi, 3 - 3 * hi)))

    def copy(self, send_kind, recv, i, t, r, s, dev):
        size = self.rows if s is None else self.rows // self.subs
        block = self.slots.at[t, r, pl.ds(0 if s is None else s * size, size)]
        return pltpu.make_async_remote_copy(
            src_ref=block, dst_ref=block, send_sem=self.sends.at[send_kind, i], recv_sem=recv, device_id=dev, device_id_type=MESH)

    def near(self, i, t, s=None):
        return self.copy(0, self.recvs.at[0, t, s or 0], i, t, self.p.r, s, self.p.near)

    def far(self, i, t, s=None):
        return self.copy(1, self.recvs.at[0, t, s or 0], i, t, self.p.r, s, self.p.far)

    def cross(self, i, t, s=None):
        return self.copy(2, self.recvs.at[1, t, s or 0], i, t, self.p.r, s, self.p.across_id)

    def mate(self, i, t, s=None):
        return self.copy(3, self.mate_recvs.at[0, t], i, t, self.p.r, s, self.p.mate_id)

    def mate_across(self, i, t, s=None):
        return self.copy(4, self.mate_recvs.at[1, t], i, t, self.p.across, s, self.p.mate_id)

    def start_line(self, s):
        self.near(0, self.p.z, s).start()

        @pl.when(self.p.inner)
        def _():
            self.far(0, self.p.z, s).start()

    def start_plane(self, s):
        self.cross(0, self.p.z, s).start()
        if self.mate_recvs is not None:
            self.mate(0, self.p.z, s).start()

    def step(self, i, s):
        t = self.order(i)
        self.near(i, t, s).wait_recv()

        @pl.when(self.p.inner)
        def _():
            @pl.when(i == 1)
            def _():
                self.far(i, t, s).start()

            @pl.when(i != 1)
            def _():
                self.near(i, t, s).start()

        self.cross(i, t, s).start()
        if self.mate_recvs is not None:
            self.mate(i, t, s).start()

    def pass_across(self, i, s):
        t = self.order(i)
        self.cross(i, t, s).wait_recv()
        if self.mate_recvs is not None:
            self.mate_across(i, t, s).start()

    def wait_same(self, i):
        self.mate(i, self.order(i)).wait_recv()

    def wait_across(self, i):
        self.mate_across(i, self.order(i)).wait_recv()

    def finish(self):
        self.near(0, self.p.z).wait_send()

        @pl.when(self.p.inner)
        def _():
            for i in range(4):
                (self.far if i < 2 else self.near)(i, self.order(i)).wait_send()

        for i in range(4):
            t = self.order(i)
            self.cross(i, t).wait_send()
            if self.mate_recvs is not None:
                self.mate(i, t).wait_send()
                self.mate_across(i, t).wait_send()


def slot_codes(mask_row):
    n = mask_row.shape[1]
    upper = (lax.broadcasted_iota(jnp.int32, (n, n), 0) <= lax.broadcasted_iota(jnp.int32, (n, n), 1)).astype(F32)
    mask_f = jnp.broadcast_to(mask_row.astype(F32), (8, n))
    rank = nn(mask_f, upper)[0:1]
    return jnp.where(mask_row == 1, rank - 1.0, float(SLOTS))


def one_hot(code_row, rows):
    ids = lax.broadcasted_iota(jnp.int32, (rows, code_row.shape[1]), 0).astype(F32)
    return (ids == code_row).astype(BF16)


def column(row):
    return jnp.transpose(jnp.broadcast_to(row, (BLK, row.shape[1])))


def attend(keys, vals, qtm, state):
    top_ref, tot_ref, acc_ref, sc_ref, pr_ref = state
    n = keys.shape[0]
    ones = jnp.ones((16, n), BF16)
    scale = 32 ** -0.5
    highs = []
    for pair in range(8):
        cols = slice(BLK * (pair // 2), BLK * (pair // 2) + BLK)
        sc = nn(keys[:, cols], qtm[pair])
        sc_ref[pair, 0:n] = sc
        highs.append(jnp.max(sc, axis=0, keepdims=True))
    keeps = []
    for pair in range(8):
        old = top_ref[pair:pair + 1, :]
        new = jnp.maximum(old, highs[pair])
        top_ref[pair:pair + 1, :] = new
        keeps.append(jnp.exp((old - new) * scale))
        pr_ref[pair, 0:n] = jnp.exp((sc_ref[pair, 0:n] - new) * scale).astype(BF16)
    for pair in range(8):
        o = nn(jnp.concatenate([vals[64 * pair:64 * pair + 64], ones], axis=0), pr_ref[pair, 0:n])
        keep = keeps[pair]
        tot_ref[pair:pair + 1, :] = tot_ref[pair:pair + 1, :] * keep + o[64:65]
        a, b = slice(64 * pair, 64 * pair + 32), slice(64 * pair + 32, 64 * pair + 64)
        acc_ref[a, :] = acc_ref[a, :] * keep[:, 0:BLK] + o[0:32, 0:BLK]
        acc_ref[b, :] = acc_ref[b, :] * keep[:, BLK:256] + o[32:64, BLK:256]


def dec_front(l, a, vec_ref, wqkv, qtm, vbias, top_ref, tot_ref, acc_ref):
    row = lambda i: vec_ref[i, l:l + 1, :]
    qt = (nt(wqkv[l, 0:D], a) + column(row(4))).astype(BF16)
    vbias[...] = column(row(5))
    qtm[...] = jnp.zeros((8, BLK, 256), BF16)
    for head in range(16):
        base = 32 * (head % 4)
        qtm[head // 2, base:base + 32, BLK * (head % 2):BLK * (head % 2) + BLK] = qt[32 * head:32 * head + 32]
    top_ref[...] = jnp.full((8, 256), -jnp.inf, F32)
    tot_ref[...] = jnp.zeros((8, 256), F32)
    acc_ref[...] = jnp.zeros((D, BLK), F32)


def dec_keys(l, a, wqkv, vbias):
    keys = nt(a, wqkv[l, D:1024]).astype(BF16)
    vals = (nt(wqkv[l, 1024:3 * D], a) + jnp.concatenate([vbias[...]] * (a.shape[0] // BLK), axis=1)).astype(BF16)
    return keys, vals


def dec_back(l, h, vec_ref, wo, w1, w2, tot_ref, acc_ref):
    row = lambda i: vec_ref[i, l:l + 1, :]
    parts = []
    for head in range(16):
        inv = 1.0 / tot_ref[head // 2:head // 2 + 1, BLK * (head % 2):BLK * (head % 2) + BLK]
        parts.append((acc_ref[32 * head:32 * head + 32, :] * inv).astype(BF16))
    att = jnp.concatenate(parts, axis=0)
    res = (h.astype(F32) + tn(att, wo[l]) + row(6)).astype(BF16)
    b = layer_norm(res, row(2), row(3)).astype(BF16)
    acc = res.astype(F32) + row(7)
    for j in range(4):
        cols = pl.ds(D * j, D)
        m = gelu(nn(b, w1[l, :, cols]) + row(8 + j)).astype(BF16)
        acc = acc + nn(m, w2[l, cols, :])
    return acc.astype(BF16)


def kernel(mask_hbm, patches_hbm, pos_hbm, dpos_hbm, b_embed_hbm, evec_hbm, efin_hbm, mtok_hbm, dvec_hbm, dfin_hbm,
           w_embed_hbm, ewqkv_hbm, ewo_hbm, ew1_hbm, ew2_hbm, wdec_hbm, dwqkv_hbm, dwo_hbm, dw1_hbm, dw2_hbm,
           out_ref,
           mask_ref, patches_ref, pos_ref, dpos_ref, b_embed_ref, evec_ref, efin_ref, mtok_ref, dvec_ref, dfin_ref,
           w_embed, ewqkv, ewo, ew1, ew2, wdec, dwqkv, dwo, dw1, dw2, wsem,
           e_buf, p1_buf, e2_buf, p2_buf, f_all, att, ek, ev, zall, xsem, tsem, usem,
           dall, a_all, table, qtm, vbias, top_ref, tot_ref, acc_ref, sc_ref, pr_ref, s1, r1, m1, s2, r2, m2):
    p = Peers()
    p.greet()
    loads = {}
    state = (top_ref, tot_ref, acc_ref, sc_ref, pr_ref)
    plan = [("mask", mask_hbm, mask_ref), ("patches", patches_hbm, patches_ref), ("pos", pos_hbm, pos_ref), ("dpos", dpos_hbm, dpos_ref),
            ("bias", b_embed_hbm, b_embed_ref), ("embed", w_embed_hbm, w_embed),
            ("evec", evec_hbm, evec_ref), ("efin", efin_hbm, efin_ref), ("mtok", mtok_hbm, mtok_ref), ("dvec", dvec_hbm, dvec_ref), ("dfin", dfin_hbm, dfin_ref)]
    soon = [name for name, *_ in plan]
    for l in range(2):
        plan += [((n, l), src.at[l], dst.at[l]) for n, src, dst in (("eqkv", ewqkv_hbm, ewqkv), ("eo", ewo_hbm, ewo), ("e1", ew1_hbm, ew1), ("e2", ew2_hbm, ew2))]
    plan += [("dec", wdec_hbm, wdec)]
    for l in range(2):
        plan += [((n, l), src.at[l], dst.at[l]) for n, src, dst in (("dqkv", dwqkv_hbm, dwqkv), ("do", dwo_hbm, dwo), ("d1", dw1_hbm, dw1), ("d2", dw2_hbm, dw2))]
    for i, (name, src, dst) in enumerate(plan):
        loads[name] = pltpu.make_async_copy(src, dst, wsem.at[i])
    for name in soon:
        loads[name].start()
    loads["mask"].wait()
    code = slot_codes(mask_ref[...])
    sel = one_hot(code, SLOTS)
    have = jnp.sum(sel.astype(F32), axis=1, keepdims=True)
    loads["patches"].wait()
    picked = nn(sel, patches_ref[...]).astype(BF16)
    loads["pos"].wait()
    pos = nn(sel, pos_ref[...])
    loads["bias"].wait()
    loads["embed"].wait()
    for name, *_ in plan[len(soon):]:
        loads[name].start()
    emb = nn(picked, w_embed[...]) + b_embed_ref[...].reshape(1, E) + pos
    e_buf[...] = jnp.where(have > 0.5, emb, 0.0).astype(BF16)
    for name in ("dpos", "evec", "efin", "mtok", "dvec", "dfin"):
        loads[name].wait()
    dall[p.z, p.r, 0:BLK, :] = dpos_ref[...]
    dall[p.z, p.r, BLK:CODE, :] = jnp.broadcast_to(jnp.concatenate([code, jnp.zeros((1, 384), F32)], axis=1), (CODE - BLK, D)).astype(BF16)
    p.barrier()
    mate, across = p.mate_id, p.across_id
    first = remote(e_buf, p1_buf, xsem, 0, mate)
    first.start()
    first.wait_recv()
    both = e_buf[...].astype(F32) + p1_buf[...].astype(F32)
    e2_buf[...] = both.astype(BF16).reshape(2, 32, E)
    def part(s):
        return pl.ds(PART * s, PART)

    g1 = Gather(p, dall, s1, r1, m1, CODE, 1)
    second = [
        pltpu.make_async_remote_copy(
            src_ref=e2_buf.at[p.core, part(s)], dst_ref=p2_buf.at[part(s)], send_sem=usem.at[0, s], recv_sem=usem.at[1, s],
            device_id=across, device_id_type=MESH) for s in (0, 1)]
    for c in second:
        c.start()

    def half_block(j, t, s):
        block = f_all.at[t, p.core, part(s)]
        return pltpu.make_async_remote_copy(
            src_ref=block, dst_ref=block, send_sem=tsem.at[0, j, s], recv_sem=tsem.at[1, t, s],
            device_id={"time": g1.order(j), "region": p.r}, device_id_type=MESH)

    for s in (0, 1):
        second[s].wait_recv()
        f_all[p.z, p.core, part(s)] = (e2_buf[p.core, part(s)].astype(F32) + p2_buf[part(s)].astype(F32)).astype(BF16)
        for j in (3, 2, 1):
            half_block(j, p.z, s).start()
    g1.start_line(0)
    g1.start_plane(0)
    first.wait_send()
    for s in (0, 1):
        second[s].wait_send()
        for j in (1, 2, 3):
            half_block(j, g1.order(j), s).wait_recv()
            half_block(j, p.z, s).wait_send()
    h = jnp.concatenate([f_all[t, p.core] for t in range(4)], axis=0)
    lane = lax.broadcasted_iota(jnp.int32, (BLK, BLK), 1)
    for l in range(2):
        row = lambda i: evec_ref[i, l:l + 1, :]
        a = layer_norm(h, row(0), row(1)).astype(BF16)
        loads["eqkv", l].wait()
        ek[l, 0] = nt(ewqkv[l, E:2 * E], a).astype(BF16)
        to_mate = [remote(ek.at[l, 0], ek.at[l, 1], xsem, 2 + 2 * l, mate), remote(ev.at[l, 0], ev.at[l, 1], xsem, 3 + 2 * l, mate)]
        ev[l, 0] = (nt(a, ewqkv[l, 2 * E:3 * E]) + row(5)).astype(BF16)
        for c in to_mate:
            c.start()
        q = nt(a, ewqkv[l, 0:E]) + row(4)
        for c in to_mate:
            c.wait()
        for g in range(6):
            cols = slice(BLK * g, BLK * g + BLK)
            k = jnp.concatenate([ek[l, 0, cols, :], ek[l, 1, cols, :]], axis=1)
            v = jnp.concatenate([ev[l, 0, :, cols], ev[l, 1, :, cols]], axis=0)
            outs = []
            for s in range(2):
                qm = jnp.where((lane // 64) == s, q[:, cols], 0.0).astype(BF16)
                sc = nn(qm, k)
                top = jnp.max(sc, axis=-1, keepdims=True)
                pr = jnp.exp((sc - top) * 0.125)
                tot = jnp.sum(pr, axis=-1, keepdims=True)
                outs.append(nn(pr.astype(BF16), v) * (1.0 / tot))
            att[:, cols] = jnp.where(lane < 64, outs[0], outs[1]).astype(BF16)
        if l == 0:
            g1.step(1, 0)

            @pl.when(p.inner)
            def _():
                g1.step(2, 0)

            g1.pass_across(0, 0)
        else:
            @pl.when(p.inner)
            def _():
                g1.step(3, 0)

            @pl.when(jnp.logical_not(p.inner))
            def _():
                g1.step(2, 0)

            g1.pass_across(1, 0)
        loads["eo", l].wait()
        res = (h.astype(F32) + nn(att[...], ewo[l]) + row(6)).astype(BF16)
        b = layer_norm(res, row(2), row(3)).astype(BF16)
        acc = res.astype(F32) + row(7)
        loads["e1", l].wait()
        loads["e2", l].wait()
        for j in range(4):
            cols = pl.ds(E * j, E)
            m = gelu(nn(b, ew1[l, :, cols]) + row(8 + j)).astype(BF16)
            acc = acc + nn(m, ew2[l, cols, :])
        h = acc.astype(BF16)
    loads["dec"].wait()
    zf = layer_norm(h, efin_ref[0:1, :], efin_ref[1:2, :]).astype(BF16)
    zall[p.core] = nn(zf, wdec[...]).astype(BF16).reshape(4, 32, D)
    zcopy = remote(zall.at[p.core], zall.at[p.core], xsem, 6, mate)
    zcopy.start()
    table[:, SLOTS:ZROWS, :] = jnp.broadcast_to(mtok_ref[...].astype(F32).reshape(1, 1, D), (4, ZROWS - SLOTS, D)).astype(BF16)
    zcopy.wait()
    for half in range(2):
        table[:, 32 * half:32 * half + 32, :] = zall[half]
    def token_rows(code, t, dpos):
        return (tn(one_hot(code, ZROWS), table[t]) + dpos.astype(F32)).astype(BF16)

    h = token_rows(slot_codes(mask_ref[...]), p.z, dpos_ref[...])
    loads["dqkv", 0].wait()
    dec_front(0, layer_norm(h, dvec_ref[0, 0:1, :], dvec_ref[1, 0:1, :]).astype(BF16), dvec_ref, dwqkv, qtm, vbias, top_ref, tot_ref, acc_ref)

    @pl.when(jnp.logical_not(p.inner))
    def _():
        g1.step(3, 0)
    def norm_rows(t, r):
        u = token_rows(dall[t, r, BLK:CODE, 0:BLK].astype(F32)[0:1], t, dall[t, r, 0:BLK, :])
        return layer_norm(u, dvec_ref[0, 0:1, :], dvec_ref[1, 0:1, :]).astype(BF16)

    def first_layer(i, carry):
        t = g1.order(i)

        @pl.when((i == 1) | (i == 2))
        def _():
            g1.pass_across(i + 1, 0)

        g1.wait_same(i)
        g1.wait_across(i)
        a = jnp.concatenate([norm_rows(t, r) for r in range(4)], axis=0)
        keys, vals = dec_keys(0, a, dwqkv, vbias)
        attend(keys, vals, qtm, state)
        return carry
    lax.fori_loop(0, 4, first_layer, 0)
    for n in ("do", "d1", "d2"):
        loads[n, 0].wait()
    h = dec_back(0, h, dvec_ref, dwo, dw1, dw2, tot_ref, acc_ref)
    g1.finish()
    a_all[p.z, p.r] = layer_norm(h, dvec_ref[0, 1:2, :], dvec_ref[1, 1:2, :]).astype(BF16)
    g2 = Gather(p, a_all, s2, r2, m2, BLK, SUBS)
    for s in range(SUBS):
        g2.start_line(s)
        g2.start_plane(s)
    loads["dqkv", 1].wait()
    dec_front(1, a_all[p.z, p.r], dvec_ref, dwqkv, qtm, vbias, top_ref, tot_ref, acc_ref)
    def chunk(i, half):
        t = g2.order(i)
        ra = lax.rem(p.r + 2 * half, 4)
        rb = lax.rem(p.mate + 2 * half, 4)
        keys, vals = dec_keys(1, jnp.concatenate([a_all[t, ra], a_all[t, rb]], axis=0), dwqkv, vbias)
        attend(keys, vals, qtm, state)

    def outer_step(i, s):
        @pl.when(jnp.logical_not(p.inner))
        def _():
            g2.step(i, s)

    def inner_step(i, s):
        @pl.when(p.inner)
        def _():
            g2.step(i, s)
    g2.wait_same(0)
    chunk(0, 0)
    for s in range(SUBS):
        g2.step(1, s)
        inner_step(2, s)
        g2.pass_across(0, s)
    for s in range(SUBS):
        inner_step(3, s)
    g2.wait_across(0)
    chunk(0, 1)
    for s in range(SUBS):
        outer_step(2, s)
    g2.wait_same(1)
    chunk(1, 0)
    for s in range(SUBS):
        g2.pass_across(1, s)
    g2.wait_same(2)
    chunk(2, 0)
    for s in range(SUBS):
        outer_step(3, s)
    g2.wait_across(1)
    chunk(1, 1)
    for s in range(SUBS):
        g2.pass_across(2, s)
    g2.wait_same(3)
    chunk(3, 0)
    g2.wait_across(2)
    chunk(2, 1)
    for s in range(SUBS):
        g2.pass_across(3, s)
    g2.wait_across(3)
    chunk(3, 1)
    for n in ("do", "d1", "d2"):
        loads[n, 1].wait()
    h = dec_back(1, h, dvec_ref, dwo, dw1, dw2, tot_ref, acc_ref)
    out_ref[...] = layer_norm(h, dfin_ref[0:1, :], dfin_ref[1:2, :]).astype(BF16)
    g2.finish()


VM = pl.BlockSpec(memory_space=pltpu.VMEM)
ANY = pl.BlockSpec(memory_space=pl.ANY)
DMA = pltpu.SemaphoreType.DMA


def solution(mesh):
    def local_step(patches, enc_pos, vis_mask, dec_pos, w_embed, b_embed, enc_vec, enc_wqkv, enc_wo, enc_w1, enc_w2, enc_final, w_dec_in, mask_token, dec_vec, dec_wqkv, dec_wo, dec_w1, dec_w2, dec_final, w_out):
        mask_row = vis_mask.reshape(1, BLK)
        wq_e = jnp.transpose(enc_wqkv, (0, 2, 3, 4, 1)).reshape(2, 3 * E, E)
        wq_d = jnp.transpose(dec_wqkv, (0, 2, 3, 4, 1)).reshape(2, 3 * D, D)
        wo_e = enc_wo.reshape(2, E, E)
        wo_d = dec_wo.reshape(2, D, D)
        vm = lambda *shape: pltpu.VMEM(shape, BF16)
        vf = lambda *shape: pltpu.VMEM(shape, F32)
        y = pl.pallas_call(
            kernel,
            out_shape=pltpu.VMEM((BLK, D), BF16),
            in_specs=[ANY] * 20,
            out_specs=VM,
            scratch_shapes=[
                pltpu.VMEM((1, BLK), jnp.int32), vm(BLK, E), vm(BLK, E), vm(BLK, D), vf(E), vf(12, 2, E), vf(2, E), vm(D), vf(12, 2, D), vf(2, D),
                vm(E, E), vm(2, 3 * E, E), vm(2, E, E), vm(2, E, 4 * E), vm(2, 4 * E, E), vm(E, D),
                vm(2, 3 * D, D), vm(2, D, D), vm(2, D, 4 * D), vm(2, 4 * D, D), DMA((28,)),
                vm(64, E), vm(64, E), vm(2, 32, E), vm(32, E), vm(4, 2, 32, E), vm(BLK, E), vm(2, 2, E, BLK), vm(2, 2, BLK, E), vm(2, 4, 32, D), DMA((2, 7)), DMA((2, 4, 2)), DMA((2, 2)),
                vm(4, 4, CODE, D), vm(4, 4, BLK, D), vm(4, ZROWS, D), vm(8, BLK, 256), vf(D, BLK), vf(8, 256), vf(8, 256), vf(D, BLK), vf(8, D, 256), vm(8, D, 256),
                *Gather.sems(1, True), *Gather.sems(SUBS, True),
            ],
            compiler_params=pltpu.CompilerParams(collective_id=0, has_side_effects=True, vmem_limit_bytes=61 * 1024 * 1024),
            name="mae",
        )(mask_row, patches, enc_pos, dec_pos, b_embed, jnp.transpose(enc_vec, (1, 0, 2)), enc_final,
          mask_token, jnp.transpose(dec_vec, (1, 0, 2)), dec_final,
          w_embed, wq_e, wo_e, enc_w1, enc_w2, w_dec_in, wq_d, wo_d, dec_w1, dec_w2)
        return jnp.dot(y, w_out, preferred_element_type=F32)

    token_rows = P(TOKEN_AXES, None)
    token_flags = P(TOKEN_AXES)
    replicated = P()
    in_specs = (token_rows, token_rows, token_flags, token_rows) + (replicated,) * 17
    return jax.shard_map(local_step, mesh=mesh, in_specs=in_specs, out_specs=token_rows, check_vma=False)
```
